16 devices in a mesh: dp: 2 (over y, z), ep: 8 (over x, core).
Axes of the slice: x: 4, y: 2, z: 1, core: 2. Of those that a mesh axis runs over, the one named last changes fastest.
The devices are a block of a 4x4x8 slice.
Arguments:
- tokens: bfloat16 [131072, 768], P(('dp', 'ep')), parts along dimension 0
- expert_idx: int32 [131072], P(('dp', 'ep')), parts along dimension 0
- w_router: float32 [768, 64], replicated
- w_in: bfloat16 [64, 768, 3072], P('ep')
- w_out: bfloat16 [64, 3072, 768], P('ep')
Outputs:
- output: bfloat16 [131072, 768], P(('dp', 'ep')), parts along dimension 0
There are 2 independent parts. The reference program is written for one: setup_inputs(seed, part) draws one part's arguments, and reference() takes and returns one part's arrays. A program takes and returns all parts, laid end to end along the dimension named above; an argument that names none is the same for every part.
All inputs are finite; a program needn't handle non-finite values.
Results may differ from the reference program's by a relative error of at most 0.001.
Values are sent between devices in bfloat16 or wider.
A program may use at most 768 MiB of HBM per device.

```python
import jax
import jax.numpy as jnp
from jax import lax

MODEL_DIM = 768
HIDDEN_DIM = 3072
NUM_EXPERTS = 64
GROUP_TOKENS = 8192
NUM_GROUPS = 8
CAPACITY = (5 * GROUP_TOKENS + 4 * NUM_EXPERTS - 1) // (4 * NUM_EXPERTS)
TOTAL_TOKENS = NUM_GROUPS * GROUP_TOKENS


def draw_choices(key):
    key_perm, key_shift, key_redraw, key_pick, key_hot = jax.random.split(key, 5)
    balanced = jnp.arange(GROUP_TOKENS, dtype=jnp.int32) % NUM_EXPERTS
    perm_keys = jax.random.split(key_perm, NUM_GROUPS)
    shuffled = jax.vmap(lambda perm_key: jax.random.permutation(perm_key, balanced))(perm_keys)
    group_shift = jax.random.randint(key_shift, (NUM_GROUPS, 1), 0, NUM_EXPERTS)
    choice = (shuffled + group_shift) % NUM_EXPERTS
    redraw = jax.random.randint(key_redraw, (NUM_GROUPS, GROUP_TOKENS), 0, 8) == 0
    picked = jax.random.randint(key_pick, (NUM_GROUPS, GROUP_TOKENS), 0, NUM_EXPERTS)
    choice = jnp.where(redraw, picked, choice)
    hot_expert = jax.random.randint(key_hot, (NUM_GROUPS, 1), 0, NUM_EXPERTS)
    leading = jnp.arange(GROUP_TOKENS)[None, :] <= CAPACITY
    choice = jnp.where(leading, hot_expert, choice)
    return choice.reshape(TOTAL_TOKENS).astype(jnp.int32)


def expert_weights(key, fan_in, fan_out, weight_scale):
    expert_keys = jax.random.split(key, NUM_EXPERTS)
    return lax.map(lambda one_key: (jax.random.normal(one_key, (fan_in, fan_out), jnp.float32) * weight_scale).astype(jnp.bfloat16), expert_keys)


def setup_inputs(seed: int = 0, part: int = 0) -> dict:
    root_key = jax.random.key(seed)
    key_tokens, key_choice, key_router, key_in, key_out = jax.random.split(root_key, 5)
    tokens = jax.random.normal(jax.random.fold_in(key_tokens, part), (TOTAL_TOKENS, MODEL_DIM), jnp.float32).astype(jnp.bfloat16)
    expert_idx = draw_choices(jax.random.fold_in(key_choice, part))
    w_router = jax.random.normal(key_router, (MODEL_DIM, NUM_EXPERTS), jnp.float32) * MODEL_DIM ** -0.5
    w_in = expert_weights(key_in, MODEL_DIM, HIDDEN_DIM, MODEL_DIM ** -0.5)
    w_out = expert_weights(key_out, HIDDEN_DIM, MODEL_DIM, NUM_EXPERTS * HIDDEN_DIM ** -0.5)
    return {"tokens": tokens, "expert_idx": expert_idx, "w_router": w_router, "w_in": w_in, "w_out": w_out}


def route_group(tok_rows, choice, w_router):
    logits = jnp.dot(tok_rows.astype(jnp.float32), w_router, precision=lax.Precision.HIGHEST)
    router_prob = jax.nn.softmax(logits, axis=-1)
    chosen = choice[:, None] == jnp.arange(NUM_EXPERTS, dtype=jnp.int32)[None, :]
    gate_prob = jnp.sum(jnp.where(chosen, router_prob, 0.0), axis=-1)
    running_count = jnp.cumsum(chosen.astype(jnp.int32), axis=0) - 1
    position = jnp.sum(jnp.where(chosen, running_count, 0), axis=-1)
    slot_index = jnp.where(position < CAPACITY, choice * CAPACITY + position, NUM_EXPERTS * CAPACITY)
    holder = jnp.full((NUM_EXPERTS * CAPACITY + 1,), GROUP_TOKENS, jnp.int32).at[slot_index].set(jnp.arange(GROUP_TOKENS, dtype=jnp.int32))
    buffer = jnp.take(tok_rows, holder[:-1], axis=0, mode="fill", fill_value=0)
    return buffer.reshape(NUM_EXPERTS, CAPACITY, MODEL_DIM), slot_index, gate_prob


def expert_apply(operands):
    rows_in, weight_in, weight_out = operands
    hidden = jnp.dot(rows_in, weight_in, preferred_element_type=jnp.float32)
    hidden_act = jax.nn.relu(hidden).astype(jnp.bfloat16)
    return jnp.dot(hidden_act, weight_out, preferred_element_type=jnp.float32).astype(jnp.bfloat16)


def combine_group(operands):
    flat_out, slot_rows, gate_rows = operands
    picked = jnp.take(flat_out, slot_rows, axis=0, mode="fill", fill_value=0)
    return (gate_rows[:, None] * picked.astype(jnp.float32)).astype(jnp.bfloat16)


def reference(tokens, expert_idx, w_router, w_in, w_out):
    grouped = tokens.reshape(NUM_GROUPS, GROUP_TOKENS, MODEL_DIM)
    choices = expert_idx.reshape(NUM_GROUPS, GROUP_TOKENS)
    buffers, slot_index, gate_prob = lax.map(lambda pair: route_group(pair[0], pair[1], w_router), (grouped, choices))
    per_expert = jnp.swapaxes(buffers, 0, 1).reshape(NUM_EXPERTS, NUM_GROUPS * CAPACITY, MODEL_DIM)
    expert_rows = lax.map(expert_apply, (per_expert, w_in, w_out))
    by_group = jnp.swapaxes(expert_rows.reshape(NUM_EXPERTS, NUM_GROUPS, CAPACITY, MODEL_DIM), 0, 1).reshape(NUM_GROUPS, NUM_EXPERTS * CAPACITY, MODEL_DIM)
    outputs = lax.map(combine_group, (by_group, slot_index, gate_prob))
    return outputs.reshape(TOTAL_TOKENS, MODEL_DIM)
```

```python
import functools

import jax
import jax.numpy as jnp
from jax import lax
from jax.experimental import pallas as pl
from jax.experimental.pallas import tpu as pltpu
from jax.sharding import PartitionSpec as P

MESH = pl.DeviceIdType.MESH
F_TILE = 512
N_TILE = 256


def route(choice, num_experts, capacity):
    tok_count = choice.shape[0]
    chunk = 256
    parts = tok_count // chunk
    chosen = (choice[:, None] == jnp.arange(num_experts, dtype=jnp.int32)[None, :])
    ones = chosen.astype(jnp.bfloat16).reshape(parts, chunk, num_experts)
    lower = jnp.tril(jnp.ones((chunk, chunk), jnp.bfloat16))
    inside = jnp.einsum("st,cte->cse", lower, ones, preferred_element_type=jnp.float32)
    totals = inside[:, -1, :]
    before = jnp.cumsum(totals, axis=0) - totals
    running = (inside + before[:, None, :] - 1.0).reshape(tok_count, num_experts)
    position = jnp.sum(jnp.where(chosen, running, 0.0), axis=-1).astype(jnp.int32)
    slot_index = jnp.where(position < capacity, choice * capacity + position, num_experts * capacity)
    holder = jnp.full((num_experts * capacity + 1,), tok_count, jnp.int32).at[slot_index].set(jnp.arange(tok_count, dtype=jnp.int32))
    return slot_index, holder[:-1]


def gate_of(tok_rows, choice, w_router):
    num_experts = w_router.shape[1]
    logits = jnp.dot(tok_rows.astype(jnp.float32), w_router, precision=lax.Precision.HIGHEST)
    router_prob = jax.nn.softmax(logits, axis=-1)
    chosen = choice[:, None] == jnp.arange(num_experts, dtype=jnp.int32)[None, :]
    return jnp.sum(jnp.where(chosen, router_prob, 0.0), axis=-1)


def peer_order(groups):
    return tuple(range(1, groups))


def exchange_kernel(groups, send_buf, w_in, w_out, back_buf, rows, win_buf, wout_buf, hidden,
                    dsend, drecv, rsend, rrecv, own_in, own_out, wsem):
    me = lax.axis_index("ep")
    local_experts = w_in.shape[0]
    cap = send_buf.shape[2]
    hidden_dim = w_in.shape[2]
    model_dim = w_in.shape[1]
    peers = peer_order(groups)

    barrier = pltpu.get_barrier_semaphore()
    for dist in peers:
        pl.semaphore_signal(barrier, inc=1, device_id={"ep": lax.rem(me + dist, groups)}, device_id_type=MESH)
    pl.semaphore_wait(barrier, groups - 1)

    def out_copy(k, dist):
        to = lax.rem(me + dist, groups)
        return pltpu.make_async_remote_copy(
            src_ref=send_buf.at[to, k], dst_ref=rows.at[k, pl.ds(pl.multiple_of(me * cap, cap), cap)],
            send_sem=dsend.at[dist, k], recv_sem=drecv.at[dist, k], device_id={"ep": to}, device_id_type=MESH)

    def own_copy(k):
        return pltpu.make_async_copy(send_buf.at[me, k], rows.at[k, pl.ds(pl.multiple_of(me * cap, cap), cap)], own_in.at[k])

    def back_copy(k, dist):
        to = lax.rem(me + dist, groups)
        return pltpu.make_async_remote_copy(
            src_ref=rows.at[k, pl.ds(pl.multiple_of(to * cap, cap), cap)], dst_ref=back_buf.at[me, k],
            send_sem=rsend.at[dist, k], recv_sem=rrecv.at[dist, k], device_id={"ep": to}, device_id_type=MESH)

    def own_back(k):
        return pltpu.make_async_copy(rows.at[k, pl.ds(pl.multiple_of(me * cap, cap), cap)], back_buf.at[me, k], own_out.at[k])

    def weights(k, slot):
        return (pltpu.make_async_copy(w_in.at[k], win_buf.at[slot], wsem.at[0, slot]),
                pltpu.make_async_copy(w_out.at[k], wout_buf.at[slot], wsem.at[1, slot]))

    def start_sends(k, carry):
        for dist in peers:
            out_copy(k, dist).start()
        own_copy(k).start()
        return carry

    lax.fori_loop(0, local_experts, start_sends, 0)
    for cp in weights(0, 0):
        cp.start()

    def expert(k, carry):
        slot = lax.rem(k, 2)

        @pl.when(k + 1 < local_experts)
        def _():
            for cp in weights(k + 1, 1 - slot):
                cp.start()

        for dist in peers:
            out_copy(k, dist).wait_recv()
        own_copy(k).wait()
        for cp in weights(k, slot):
            cp.wait()

        def first(f, c):
            cols = pl.ds(pl.multiple_of(f * F_TILE, F_TILE), F_TILE)
            acc = jnp.dot(rows[k], win_buf[slot, :, cols], preferred_element_type=jnp.float32)
            hidden[:, cols] = jnp.maximum(acc, 0.0).astype(jnp.bfloat16)
            return c

        lax.fori_loop(0, hidden_dim // F_TILE, first, 0)

        def second(n, c):
            cols = pl.ds(pl.multiple_of(n * N_TILE, N_TILE), N_TILE)
            acc = jnp.dot(hidden[...], wout_buf[slot, :, cols], preferred_element_type=jnp.float32)
            rows[k, :, cols] = acc.astype(jnp.bfloat16)
            return c

        lax.fori_loop(0, model_dim // N_TILE, second, 0)
        for dist in peers:
            back_copy(k, dist).start()
        own_back(k).start()
        return carry

    lax.fori_loop(0, local_experts, expert, 0)

    def finish(k, carry):
        for dist in peers:
            out_copy(k, dist).wait_send()
        for dist in peers:
            back_copy(k, dist).wait()
        own_back(k).wait()
        return carry

    lax.fori_loop(0, local_experts, finish, 0)


def exchange(groups, send_buf, w_in, w_out):
    local_experts, model_dim, hidden_dim = w_in.shape
    cap = send_buf.shape[2]
    return pl.pallas_call(
        functools.partial(exchange_kernel, groups),
        out_shape=jax.ShapeDtypeStruct((groups, local_experts, cap, model_dim), jnp.bfloat16),
        in_specs=[pl.BlockSpec(memory_space=pl.ANY)] * 3,
        out_specs=pl.BlockSpec(memory_space=pl.ANY),
        scratch_shapes=[
            pltpu.VMEM((local_experts, groups * cap, model_dim), jnp.bfloat16),
            pltpu.VMEM((2, model_dim, hidden_dim), jnp.bfloat16),
            pltpu.VMEM((2, hidden_dim, model_dim), jnp.bfloat16),
            pltpu.VMEM((groups * cap, hidden_dim), jnp.bfloat16),
            pltpu.SemaphoreType.DMA((groups, local_experts)),
            pltpu.SemaphoreType.DMA((groups, local_experts)),
            pltpu.SemaphoreType.DMA((groups, local_experts)),
            pltpu.SemaphoreType.DMA((groups, local_experts)),
            pltpu.SemaphoreType.DMA((local_experts,)),
            pltpu.SemaphoreType.DMA((local_experts,)),
            pltpu.SemaphoreType.DMA((2, 2)),
        ],
        compiler_params=pltpu.CompilerParams(collective_id=0, has_side_effects=True, vmem_limit_bytes=62 * 1024 * 1024),
        name="exchange",
    )(send_buf, w_in, w_out)


def solution(mesh):
    groups = mesh.shape["ep"]

    def local_block(tokens, expert_idx, w_router, w_in, w_out):
        tok_count, model_dim = tokens.shape
        local_experts = w_in.shape[0]
        num_experts = local_experts * groups
        capacity = (5 * tok_count + 4 * num_experts - 1) // (4 * num_experts)
        slot_index, holder = route(expert_idx, num_experts, capacity)
        gate_prob = gate_of(tokens, expert_idx, w_router)
        buffer = jnp.take(tokens, holder, axis=0, mode="fill", fill_value=0)
        back_buf = exchange(groups, buffer.reshape(groups, local_experts, capacity, model_dim), w_in, w_out)
        flat_out = back_buf.reshape(num_experts * capacity, model_dim)
        picked = jnp.take(flat_out, slot_index, axis=0, mode="fill", fill_value=0)
        return (gate_prob[:, None] * picked.astype(jnp.float32)).astype(jnp.bfloat16)

    return jax.shard_map(local_block, mesh=mesh, in_specs=(P(("dp", "ep"), None), P(("dp", "ep")), P(None, None), P("ep", None, None), P("ep", None, None)), out_specs=P(("dp", "ep"), None), check_vma=False)
```

```python
import functools

import jax
import jax.numpy as jnp
from jax import lax
from jax.experimental import pallas as pl
from jax.experimental.pallas import tpu as pltpu
from jax.sharding import PartitionSpec as P

MESH = pl.DeviceIdType.MESH
LANES = 128
F_TILE = 512
N_TILE = 256
ROUTE_CHUNK = 256
TOK_TILE = 512
UNROLL = 16
VMEM_LIMIT = 62 * 1024 * 1024


def route_kernel(num_experts, capacity, width, choice_ref, holder_ref, slot_ref, keep_ref):
    parts = choice_ref.shape[0]
    chunk = choice_ref.shape[2]
    expert_ids = lax.broadcasted_iota(jnp.int32, (num_experts, chunk), 0)
    col_ids = lax.broadcasted_iota(jnp.int32, (width, chunk), 0)
    local_id = lax.broadcasted_iota(jnp.int32, (num_experts, chunk), 1).astype(jnp.float32)
    upper = (lax.broadcasted_iota(jnp.int32, (chunk, chunk), 0) <= lax.broadcasted_iota(jnp.int32, (chunk, chunk), 1)).astype(jnp.bfloat16)

    def body(c, carry):
        before, table = carry
        choice = choice_ref[c]
        hit = expert_ids == choice
        ones = hit.astype(jnp.float32)
        running = jnp.dot(ones.astype(jnp.bfloat16), upper, preferred_element_type=jnp.float32) + before
        position = (jnp.sum(ones * running, axis=0, keepdims=True) - 1.0).astype(jnp.int32)
        kept = position < capacity
        slot_ref[c] = jnp.where(kept, choice * capacity + position, 0)
        keep_ref[c] = kept.astype(jnp.float32)
        at_col = (col_ids == position).astype(jnp.float32).astype(jnp.bfloat16)
        both = jnp.concatenate([ones * local_id, ones], axis=0).astype(jnp.bfloat16)
        found = lax.dot_general(both, at_col, (((1,), (1,)), ((), ())), preferred_element_type=jnp.float32)
        table = table + found[:num_experts] + found[num_experts:] * (c * chunk).astype(jnp.float32)
        return running[:, chunk - 1:], table

    _, table = lax.fori_loop(0, parts, body, (jnp.zeros((num_experts, 1), jnp.float32), jnp.zeros((num_experts, width), jnp.float32)), unroll=2)
    holder_ref[...] = table.astype(jnp.int32)


def route(expert_idx, num_experts, capacity):
    tok_count = expert_idx.shape[0]
    parts = tok_count // ROUTE_CHUNK
    width = -(-capacity // LANES) * LANES
    shape = (parts, 1, ROUTE_CHUNK)
    return pl.pallas_call(
        functools.partial(route_kernel, num_experts, capacity, width),
        out_shape=(jax.ShapeDtypeStruct((num_experts, width), jnp.int32), jax.ShapeDtypeStruct(shape, jnp.int32), jax.ShapeDtypeStruct(shape, jnp.float32)),
        name="route",
    )(expert_idx.reshape(shape))


def exchange_kernel(groups, num_experts, cap, holder, tokens, choice, w_router, w_in, w_out, back_buf, gate_ref, send_buf,
                    rows, dsend, drecv, rsend, rrecv, own_in, own_out, wsem, tok_sem, stage_sem):
    me = lax.axis_index("ep")
    local_experts, model_dim, hidden_dim = w_in.shape
    width = holder.shape[0] // num_experts
    tok_count = tokens.shape[0]
    tok_tiles = tok_count // TOK_TILE
    pieces = model_dim // LANES
    peers = tuple(range(1, groups))
    rows_all = groups * cap

    barrier = pltpu.get_barrier_semaphore()
    for dist in peers:
        pl.semaphore_signal(barrier, inc=1, device_id={"ep": lax.rem(me + dist, groups)}, device_id_type=MESH)

    def block(i):
        return pl.ds(pl.multiple_of(i * cap, cap), cap)

    def out_copy(k, dist):
        to = lax.rem(me + dist, groups)
        return pltpu.make_async_remote_copy(
            src_ref=send_buf.at[k, block(to)], dst_ref=rows.at[k, block(me)],
            send_sem=dsend.at[dist, k], recv_sem=drecv.at[dist, k], device_id={"ep": to}, device_id_type=MESH)

    def own_copy(k):
        return pltpu.make_async_copy(send_buf.at[k, block(me)], rows.at[k, block(me)], own_in.at[k])

    def back_copy(k, dist):
        to = lax.rem(me + dist, groups)
        return pltpu.make_async_remote_copy(
            src_ref=rows.at[k, block(to)], dst_ref=back_buf.at[me, k],
            send_sem=rsend.at[dist, k], recv_sem=rrecv.at[dist, k], device_id={"ep": to}, device_id_type=MESH)

    def own_back(k):
        return pltpu.make_async_copy(rows.at[k, block(me)], back_buf.at[me, k], own_out.at[k])

    def tok_copy(i, slot, tile_ref):
        return pltpu.make_async_copy(tokens.at[pl.ds(pl.multiple_of(i * TOK_TILE, TOK_TILE), TOK_TILE)], tile_ref.at[slot], tok_sem.at[slot])

    def send_phase(tok_lin, tile_ref, picked, packed):
        depth = tile_ref.shape[0]
        for i in range(depth - 1):
            tok_copy(i, i, tile_ref).start()

        def load_tile(i, carry):
            @pl.when(i + depth - 1 < tok_tiles)
            def _():
                tok_copy(i + depth - 1, lax.rem(i + depth - 1, depth), tile_ref).start()

            slot = lax.rem(i, depth)
            tok_copy(i, slot, tile_ref).wait()
            for j in range(pieces):
                tok_lin[pl.ds(i * (TOK_TILE * pieces) + j, TOK_TILE, stride=pieces), :] = tile_ref[slot, :, j * LANES:(j + 1) * LANES].astype(jnp.float32)
            return carry

        lax.fori_loop(0, tok_tiles, load_tile, 0)
        pl.semaphore_wait(barrier, groups - 1)

        def stage_copy(k):
            slot = lax.rem(k, 2)
            return pltpu.make_async_copy(packed.at[slot], send_buf.at[k], stage_sem.at[slot])

        def send(k):
            stage_copy(k).wait()
            for dist in peers:
                out_copy(k, dist).start()
            own_copy(k).start()

        def gather(k, carry):
            def one_dest(j, c):
                first_slot = (j * local_experts + k) * width

                def some(q, cc):
                    for u in range(UNROLL):
                        at = q * UNROLL + u
                        tok = holder[first_slot + at]
                        picked[pl.ds((j * cap + at) * pieces, pieces), :] = tok_lin[pl.ds(tok * pieces, pieces), :]
                    return cc

                return lax.fori_loop(0, cap // UNROLL, some, c)

            lax.fori_loop(0, groups, one_dest, 0)
            slot = lax.rem(k, 2)
            for j in range(pieces):
                packed[slot, :, j * LANES:(j + 1) * LANES] = picked[pl.ds(j, rows_all, stride=pieces), :].astype(jnp.bfloat16)

            @pl.when(k > 0)
            def _():
                send(k - 1)

            stage_copy(k).start()
            return carry

        lax.fori_loop(0, local_experts, gather, 0)
        send(local_experts - 1)

    pl.run_scoped(
        send_phase,
        pltpu.VMEM((tok_count * pieces, LANES), jnp.float32),
        pltpu.VMEM((4, TOK_TILE, model_dim), jnp.bfloat16),
        pltpu.VMEM((rows_all * pieces, LANES), jnp.float32),
        pltpu.VMEM((2, rows_all, model_dim), jnp.bfloat16),
    )

    def expert_phase(win_buf, wout_buf, hidden):
        def weights(k, slot):
            return (pltpu.make_async_copy(w_in.at[k], win_buf.at[slot], wsem.at[0, slot]),
                    pltpu.make_async_copy(w_out.at[k], wout_buf.at[slot], wsem.at[1, slot]))

        for cp in weights(0, 0):
            cp.start()

        def expert(k, carry):
            slot = lax.rem(k, 2)

            @pl.when(k + 1 < local_experts)
            def _():
                for cp in weights(k + 1, 1 - slot):
                    cp.start()

            for dist in peers:
                out_copy(k, dist).wait_recv()
            own_copy(k).wait()
            for cp in weights(k, slot):
                cp.wait()

            def first(f, c):
                cols = pl.ds(pl.multiple_of(f * F_TILE, F_TILE), F_TILE)
                acc = jnp.dot(rows[k], win_buf[slot, :, cols], preferred_element_type=jnp.float32)
                hidden[:, cols] = jnp.maximum(acc, 0.0).astype(jnp.bfloat16)
                return c

            lax.fori_loop(0, hidden_dim // F_TILE, first, 0)

            def second(n, c):
                cols = pl.ds(pl.multiple_of(n * N_TILE, N_TILE), N_TILE)
                acc = jnp.dot(hidden[...], wout_buf[slot, :, cols], preferred_element_type=jnp.float32)
                rows[k, :, cols] = acc.astype(jnp.bfloat16)
                return c

            lax.fori_loop(0, model_dim // N_TILE, second, 0)
            for dist in peers:
                back_copy(k, dist).start()
            own_back(k).start()
            return carry

        lax.fori_loop(0, local_experts, expert, 0)

    pl.run_scoped(
        expert_phase,
        pltpu.VMEM((2, model_dim, hidden_dim), jnp.bfloat16),
        pltpu.VMEM((2, hidden_dim, model_dim), jnp.bfloat16),
        pltpu.VMEM((rows_all, hidden_dim), jnp.bfloat16),
    )

    def gate_phase(tile_ref):
        tok_copy(0, 0, tile_ref).start()
        expert_ids = lax.broadcasted_iota(jnp.int32, (num_experts, TOK_TILE), 0)

        def gate_tile(i, carry):
            slot = lax.rem(i, 2)

            @pl.when(i + 1 < tok_tiles)
            def _():
                tok_copy(i + 1, 1 - slot, tile_ref).start()

            tok_copy(i, slot, tile_ref).wait()
            tile = tile_ref[slot]
            part = [jnp.dot(tile, w_router[p], preferred_element_type=jnp.float32) for p in range(3)]
            logits = jnp.transpose(part[0] + (part[1] + part[2]))[:num_experts]
            weight = jnp.exp(logits - jnp.max(logits, axis=0, keepdims=True))
            own = jnp.sum(jnp.where(expert_ids == choice[i], weight, 0.0), axis=0, keepdims=True)
            gate_ref[i] = own / jnp.sum(weight, axis=0, keepdims=True)
            return carry

        lax.fori_loop(0, tok_tiles, gate_tile, 0)

    pl.run_scoped(gate_phase, pltpu.VMEM((2, TOK_TILE, model_dim), jnp.bfloat16))

    def finish(k, carry):
        for dist in peers:
            out_copy(k, dist).wait_send()
        for dist in peers:
            back_copy(k, dist).wait()
        own_back(k).wait()
        return carry

    lax.fori_loop(0, local_experts, finish, 0)


def split_router(w_router):
    pad = -w_router.shape[1] % LANES
    rest = jnp.pad(w_router, ((0, 0), (0, pad)))
    parts = []
    for _ in range(3):
        piece = lax.reduce_precision(rest, 8, 7)
        parts.append(piece.astype(jnp.bfloat16))
        rest = rest - piece
    return jnp.stack(parts)


def exchange(groups, cap, holder, tokens, choice, w_router, w_in, w_out):
    local_experts, model_dim, hidden_dim = w_in.shape
    num_experts = groups * local_experts
    tok_count = tokens.shape[0]
    tok_tiles = tok_count // TOK_TILE
    hbm = pl.BlockSpec(memory_space=pl.ANY)
    vmem = pl.BlockSpec(memory_space=pltpu.VMEM)
    return pl.pallas_call(
        functools.partial(exchange_kernel, groups, num_experts, cap),
        out_shape=(
            jax.ShapeDtypeStruct((groups, local_experts, cap, model_dim), jnp.bfloat16),
            jax.ShapeDtypeStruct((tok_tiles, 1, TOK_TILE), jnp.float32),
            jax.ShapeDtypeStruct((local_experts, groups * cap, model_dim), jnp.bfloat16),
        ),
        in_specs=[pl.BlockSpec(memory_space=pltpu.SMEM), hbm, vmem, vmem, hbm, hbm],
        out_specs=(hbm, vmem, hbm),
        scratch_shapes=[
            pltpu.VMEM((local_experts, groups * cap, model_dim), jnp.bfloat16),
            pltpu.SemaphoreType.DMA((groups, local_experts)),
            pltpu.SemaphoreType.DMA((groups, local_experts)),
            pltpu.SemaphoreType.DMA((groups, local_experts)),
            pltpu.SemaphoreType.DMA((groups, local_experts)),
            pltpu.SemaphoreType.DMA((local_experts,)),
            pltpu.SemaphoreType.DMA((local_experts,)),
            pltpu.SemaphoreType.DMA((2, 2)),
            pltpu.SemaphoreType.DMA((4,)),
            pltpu.SemaphoreType.DMA((2,)),
        ],
        compiler_params=pltpu.CompilerParams(collective_id=0, has_side_effects=True, vmem_limit_bytes=VMEM_LIMIT),
        name="exchange",
    )(holder.reshape(-1), tokens, choice.reshape(tok_tiles, 1, TOK_TILE), split_router(w_router), w_in, w_out)


def combine_kernel(in_tile, slot_ref, gate_ref, keep_ref, src_hbm, y_ref, src_lin, stage, picked, sems):
    i = pl.program_id(0)
    tile, model_dim = y_ref.shape
    pieces = model_dim // LANES
    in_tiles = src_hbm.shape[0] // in_tile
    depth = stage.shape[0]

    @pl.when(i == 0)
    def _():
        def copy(b):
            slot = lax.rem(b, depth)
            return pltpu.make_async_copy(src_hbm.at[pl.ds(pl.multiple_of(b * in_tile, in_tile), in_tile)], stage.at[slot], sems.at[slot])

        for b in range(depth - 1):
            copy(jnp.int32(b)).start()

        def load(b, carry):
            @pl.when(b + depth - 1 < in_tiles)
            def _():
                copy(b + depth - 1).start()

            copy(b).wait()
            for j in range(pieces):
                src_lin[pl.ds(b * (in_tile * pieces) + j, in_tile, stride=pieces), :] = stage[lax.rem(b, depth), :, j * LANES:(j + 1) * LANES].astype(jnp.float32)
            return carry

        lax.fori_loop(0, in_tiles, load, 0)

    def pick(q, carry):
        for u in range(UNROLL):
            at = q * UNROLL + u
            row = slot_ref[i * tile + at]
            picked[pl.ds(at * pieces, pieces), :] = src_lin[pl.ds(row * pieces, pieces), :]
        return carry

    lax.fori_loop(0, tile // UNROLL, pick, 0)
    gate_row = jnp.where(keep_ref[0] > 0.0, gate_ref[0], -1.0)
    gate = jnp.transpose(jnp.broadcast_to(gate_row, (8, tile)))[:, :1]
    for j in range(pieces):
        value = picked[pl.ds(j, tile, stride=pieces), :] * gate
        y_ref[:, j * LANES:(j + 1) * LANES] = jnp.where(gate >= 0.0, value, 0.0).astype(jnp.bfloat16)


def combine(flat_out, slot_index, gate, keep):
    row_count, model_dim = flat_out.shape
    tok_tiles, _, tile = gate.shape
    pieces = model_dim // LANES
    in_tile = 512
    row_spec = pl.BlockSpec((1, 1, tile), lambda i, s: (i, 0, 0))
    return pl.pallas_call(
        functools.partial(combine_kernel, in_tile),
        grid_spec=pltpu.PrefetchScalarGridSpec(
            num_scalar_prefetch=1,
            grid=(tok_tiles,),
            in_specs=[row_spec, row_spec, pl.BlockSpec(memory_space=pl.ANY)],
            out_specs=pl.BlockSpec((tile, model_dim), lambda i, s: (i, 0)),
            scratch_shapes=[
                pltpu.VMEM((row_count * pieces, LANES), jnp.float32),
                pltpu.VMEM((4, in_tile, model_dim), jnp.bfloat16),
                pltpu.VMEM((tile * pieces, LANES), jnp.float32),
                pltpu.SemaphoreType.DMA((4,)),
            ],
        ),
        out_shape=jax.ShapeDtypeStruct((tok_tiles * tile, model_dim), jnp.bfloat16),
        compiler_params=pltpu.CompilerParams(vmem_limit_bytes=VMEM_LIMIT),
        name="combine",
    )(slot_index.reshape(-1), gate, keep.reshape(gate.shape), flat_out)


def solution(mesh):
    groups = mesh.shape["ep"]

    def local_block(tokens, expert_idx, w_router, w_in, w_out):
        tok_count, model_dim = tokens.shape
        local_experts = w_in.shape[0]
        num_experts = local_experts * groups
        capacity = (5 * tok_count + 4 * num_experts - 1) // (4 * num_experts)
        holder, slot_index, keep = route(expert_idx, num_experts, capacity)
        back_buf, gate, _ = exchange(groups, capacity, holder, tokens, expert_idx, w_router, w_in, w_out)
        return combine(back_buf.reshape(num_experts * capacity, model_dim), slot_index, gate, keep)

    return jax.shard_map(local_block, mesh=mesh, in_specs=(P(("dp", "ep"), None), P(("dp", "ep")), P(None, None), P("ep", None, None), P("ep", None, None)), out_specs=P(("dp", "ep"), None), check_vma=False)
```

```python
import functools

import jax
import jax.numpy as jnp
from jax import lax
from jax.experimental import pallas as pl
from jax.experimental.pallas import tpu as pltpu
from jax.sharding import PartitionSpec as P

MESH = pl.DeviceIdType.MESH
LANES = 128
F_TILE = 512
N_TILE = 256
ROUTE_CHUNK = 256
TOK_TILE = 512
UNROLL = 16
VMEM_LIMIT = 62 * 1024 * 1024


def route_kernel(groups, num_experts, capacity, main, spill, choice_ref, holder_ref, ids_ref, slot_ref, full_ref, keep_ref):
    parts, _, chunk = choice_ref.shape
    local_experts = num_experts // groups
    table_rows = num_experts + groups
    expert_ids = lax.broadcasted_iota(jnp.int32, (num_experts, chunk), 0)
    row_ids = lax.broadcasted_iota(jnp.int32, (table_rows, chunk), 0)
    col_ids = lax.broadcasted_iota(jnp.int32, (LANES, chunk), 0)
    local_id = lax.broadcasted_iota(jnp.int32, (table_rows, chunk), 1).astype(jnp.float32)
    upper = (lax.broadcasted_iota(jnp.int32, (chunk, chunk), 0) <= lax.broadcasted_iota(jnp.int32, (chunk, chunk), 1)).astype(jnp.bfloat16)

    def count(c, acc):
        return acc + (expert_ids == choice_ref[c]).astype(jnp.float32)

    totals = jnp.sum(lax.fori_loop(0, parts, count, jnp.zeros((num_experts, chunk), jnp.float32), unroll=4), axis=1, keepdims=True)
    extra = jnp.clip(totals - main, 0.0, float(capacity - main))
    row = lax.broadcasted_iota(jnp.int32, (num_experts, num_experts), 0)
    col = lax.broadcasted_iota(jnp.int32, (num_experts, num_experts), 1)
    same = col < row
    for j in range(1, groups):
        same = same & ((row >= j * local_experts) == (col >= j * local_experts))
    offset = jnp.dot(same.astype(jnp.bfloat16), jnp.broadcast_to(extra, (num_experts, LANES)).astype(jnp.bfloat16), preferred_element_type=jnp.float32)[:, :1]
    too_many = jnp.max(offset + extra, axis=0, keepdims=True) > spill
    scale = 2.0 * parts * chunk

    def body(c, carry):
        before, table, ids = carry
        choice = choice_ref[c]
        ones = (expert_ids == choice).astype(jnp.float32)
        running = jnp.dot(ones.astype(jnp.bfloat16), upper, preferred_element_type=jnp.float32) + before
        packed = jnp.sum(ones * (running + (offset * scale - 1.0)), axis=0, keepdims=True).astype(jnp.int32)
        position = packed & (int(scale) - 1)
        start = (packed - position).astype(jnp.float32) * (1.0 / scale)
        dest = jnp.zeros_like(choice)
        for j in range(1, groups):
            dest = dest + (choice >= j * local_experts).astype(jnp.int32)
        kept = position < capacity
        is_main = position < main
        spill_at = start.astype(jnp.int32) + position - main
        table_row = jnp.where(is_main, choice, jnp.where(kept, num_experts + dest, table_rows))
        table_col = jnp.where(is_main, position, spill_at)
        slot_ref[c] = jnp.where(is_main, choice * main + position, jnp.where(kept, num_experts * main + dest * spill + jnp.minimum(spill_at, spill - 1), 0))
        full_ref[c] = jnp.where(kept, choice * capacity + position, num_experts * capacity)
        keep_ref[c] = kept.astype(jnp.float32)
        at_row = (row_ids == table_row).astype(jnp.float32)
        at_col = (col_ids == table_col).astype(jnp.float32).astype(jnp.bfloat16)
        local_expert = (choice - dest * local_experts).astype(jnp.float32)
        stacked = jnp.concatenate([at_row * local_id, at_row, at_row[num_experts:] * local_expert], axis=0).astype(jnp.bfloat16)
        found = lax.dot_general(stacked, at_col, (((1,), (1,)), ((), ())), preferred_element_type=jnp.float32)
        table = table + found[:table_rows] + found[table_rows:2 * table_rows] * (c * chunk).astype(jnp.float32)
        return running[:, chunk - 1:], table, ids + found[2 * table_rows:]

    init = (jnp.zeros((num_experts, 1), jnp.float32), jnp.zeros((table_rows, LANES), jnp.float32), jnp.zeros((groups, LANES), jnp.float32))
    _, table, ids = lax.fori_loop(0, parts, body, init, unroll=4)
    holder_ref[...] = table.astype(jnp.int32)
    last = lax.broadcasted_iota(jnp.int32, (groups, LANES), 1) == LANES - 1
    ids = jnp.where(last, too_many.astype(jnp.float32), ids)
    for j in range(groups):
        ids_ref[j] = jnp.broadcast_to(ids[j:j + 1], (8, LANES))


def route(expert_idx, groups, num_experts, capacity, main, spill):
    tok_count = expert_idx.shape[0]
    parts = tok_count // ROUTE_CHUNK
    shape = (parts, 1, ROUTE_CHUNK)
    return pl.pallas_call(
        functools.partial(route_kernel, groups, num_experts, capacity, main, spill),
        out_shape=(
            jax.ShapeDtypeStruct((num_experts + groups, LANES), jnp.int32),
            jax.ShapeDtypeStruct((groups, 8, LANES), jnp.float32),
            jax.ShapeDtypeStruct(shape, jnp.int32),
            jax.ShapeDtypeStruct(shape, jnp.int32),
            jax.ShapeDtypeStruct(shape, jnp.float32),
        ),
        name="route",
    )(expert_idx.reshape(shape))


def exchange_kernel(groups, num_experts, cap, spill, holder, tokens, ids, choice, w_router, w_in, w_out,
                    back_buf, gate_ref, ids_in, send_buf, send_spill,
                    rows, spill_in, spill_out, spill_expert, dsend, drecv, rsend, rrecv, own_in, own_out, isend, irecv, wsem, tok_sem, stage_sem):
    me = lax.axis_index("ep")
    local_experts, model_dim, hidden_dim = w_in.shape
    width = LANES
    tok_count = tokens.shape[0]
    tok_tiles = tok_count // TOK_TILE
    pieces = model_dim // LANES
    peers = tuple(range(1, groups))
    rows_all = groups * cap
    spill_all = groups * spill
    last = local_experts

    barrier = pltpu.get_barrier_semaphore()
    for dist in peers:
        pl.semaphore_signal(barrier, inc=1, device_id={"ep": lax.rem(me + dist, groups)}, device_id_type=MESH)

    def block(i):
        return pl.ds(pl.multiple_of(i * cap, cap), cap)

    def spill_block(i):
        return pl.ds(pl.multiple_of(i * spill, spill), spill)

    def back_block(k):
        return pl.ds(pl.multiple_of((me * local_experts + k) * cap, cap), cap)

    def back_spill(i):
        return pl.ds(pl.multiple_of(num_experts * cap + i * spill, 16), spill)

    def spill_copy(dist):
        to = lax.rem(me + dist, groups)
        return pltpu.make_async_remote_copy(
            src_ref=send_spill.at[spill_block(to)], dst_ref=spill_in.at[spill_block(me)],
            send_sem=dsend.at[dist, last], recv_sem=drecv.at[dist, last], device_id={"ep": to}, device_id_type=MESH)

    def own_spill():
        return pltpu.make_async_copy(send_spill.at[spill_block(me)], spill_in.at[spill_block(me)], own_in.at[last])

    def ids_copy(dist):
        to = lax.rem(me + dist, groups)
        return pltpu.make_async_remote_copy(
            src_ref=ids.at[to], dst_ref=ids_in.at[me],
            send_sem=isend.at[dist], recv_sem=irecv.at[dist], device_id={"ep": to}, device_id_type=MESH)

    def own_ids():
        return pltpu.make_async_copy(ids.at[me], ids_in.at[me], isend.at[0])

    def spill_back(dist):
        to = lax.rem(me + dist, groups)
        return pltpu.make_async_remote_copy(
            src_ref=spill_out.at[spill_block(to)], dst_ref=back_buf.at[back_spill(me)],
            send_sem=rsend.at[dist, last], recv_sem=rrecv.at[dist, last], device_id={"ep": to}, device_id_type=MESH)

    def own_spill_back():
        return pltpu.make_async_copy(spill_out.at[spill_block(me)], back_buf.at[back_spill(me)], own_out.at[last])

    def out_copy(k, dist):
        to = lax.rem(me + dist, groups)
        return pltpu.make_async_remote_copy(
            src_ref=send_buf.at[k, block(to)], dst_ref=rows.at[k, block(me)],
            send_sem=dsend.at[dist, k], recv_sem=drecv.at[dist, k], device_id={"ep": to}, device_id_type=MESH)

    def own_copy(k):
        return pltpu.make_async_copy(send_buf.at[k, block(me)], rows.at[k, block(me)], own_in.at[k])

    def back_copy(k, dist):
        to = lax.rem(me + dist, groups)
        return pltpu.make_async_remote_copy(
            src_ref=rows.at[k, block(to)], dst_ref=back_buf.at[back_block(k)],
            send_sem=rsend.at[dist, k], recv_sem=rrecv.at[dist, k], device_id={"ep": to}, device_id_type=MESH)

    def own_back(k):
        return pltpu.make_async_copy(rows.at[k, block(me)], back_buf.at[back_block(k)], own_out.at[k])

    def tok_copy(i, slot, tile_ref):
        return pltpu.make_async_copy(tokens.at[pl.ds(pl.multiple_of(i * TOK_TILE, TOK_TILE), TOK_TILE)], tile_ref.at[slot], tok_sem.at[slot])

    def send_phase(tok_lin, tile_ref, picked, packed):
        depth = tile_ref.shape[0]
        for i in range(depth - 1):
            tok_copy(i, i, tile_ref).start()

        def load_tile(i, carry):
            @pl.when(i + depth - 1 < tok_tiles)
            def _():
                tok_copy(i + depth - 1, lax.rem(i + depth - 1, depth), tile_ref).start()

            slot = lax.rem(i, depth)
            tok_copy(i, slot, tile_ref).wait()
            for j in range(pieces):
                tok_lin[pl.ds(i * (TOK_TILE * pieces) + j, TOK_TILE, stride=pieces), :] = tile_ref[slot, :, j * LANES:(j + 1) * LANES].astype(jnp.float32)
            return carry

        lax.fori_loop(0, tok_tiles, load_tile, 0)
        pl.semaphore_wait(barrier, groups - 1)
        for dist in peers:
            ids_copy(dist).start()
        own_ids().start()

        def pick(first_slot, first_row, n):
            def some(q, c):
                for u in range(UNROLL):
                    at = q * UNROLL + u
                    tok = holder[first_slot + at]
                    picked[pl.ds((first_row + at) * pieces, pieces), :] = tok_lin[pl.ds(tok * pieces, pieces), :]
                return c

            lax.fori_loop(0, n // UNROLL, some, 0)

        def spill_dest(j, c):
            pick((num_experts + j) * width, j * spill, spill)
            return c

        lax.fori_loop(0, groups, spill_dest, 0)
        for j in range(pieces):
            packed[1, :spill_all, j * LANES:(j + 1) * LANES] = picked[pl.ds(j, spill_all, stride=pieces), :].astype(jnp.bfloat16)
        spill_stage = pltpu.make_async_copy(packed.at[1, pl.ds(0, spill_all)], send_spill, stage_sem.at[1])
        spill_stage.start()

        def stage_copy(k):
            slot = lax.rem(k, 2)
            return pltpu.make_async_copy(packed.at[slot], send_buf.at[k], stage_sem.at[slot])

        def send(k):
            stage_copy(k).wait()
            for dist in peers:
                out_copy(k, dist).start()
            own_copy(k).start()

        def gather(k, carry):
            def one_dest(j, c):
                pick((j * local_experts + k) * width, j * cap, cap)
                return c

            lax.fori_loop(0, groups, one_dest, 0)
            slot = lax.rem(k, 2)
            for j in range(pieces):
                packed[slot, :, j * LANES:(j + 1) * LANES] = picked[pl.ds(j, rows_all, stride=pieces), :].astype(jnp.bfloat16)

            @pl.when(k > 0)
            def _():
                send(k - 1)

            @pl.when(k == 0)
            def _():
                spill_stage.wait()
                for dist in peers:
                    spill_copy(dist).start()
                own_spill().start()

            stage_copy(k).start()
            return carry

        lax.fori_loop(0, local_experts, gather, 0)
        send(local_experts - 1)

    pl.run_scoped(
        send_phase,
        pltpu.VMEM((tok_count * pieces, LANES), jnp.float32),
        pltpu.VMEM((4, TOK_TILE, model_dim), jnp.bfloat16),
        pltpu.VMEM((rows_all * pieces, LANES), jnp.float32),
        pltpu.VMEM((2, rows_all, model_dim), jnp.bfloat16),
    )

    def expert_phase(win_buf, wout_buf, hidden):
        def weights(k, slot):
            return (pltpu.make_async_copy(w_in.at[k], win_buf.at[slot], wsem.at[0, slot]),
                    pltpu.make_async_copy(w_out.at[k], wout_buf.at[slot], wsem.at[1, slot]))

        for cp in weights(0, 0):
            cp.start()
        own_ids().wait()
        own_spill().wait()
        for dist in peers:
            ids_copy(dist).wait_recv()
            spill_copy(dist).wait_recv()
        for j in range(groups):
            column = jnp.transpose(ids_in[j])[:spill, :1]
            spill_expert[spill_block(j), :] = jnp.broadcast_to(column, (spill, LANES))
        spill_out[...] = jnp.zeros_like(spill_out)

        def expert(k, carry):
            slot = lax.rem(k, 2)

            @pl.when(k + 1 < local_experts)
            def _():
                for cp in weights(k + 1, 1 - slot):
                    cp.start()

            for dist in peers:
                out_copy(k, dist).wait_recv()
            own_copy(k).wait()
            for cp in weights(k, slot):
                cp.wait()

            def first(f, c):
                cols = pl.ds(pl.multiple_of(f * F_TILE, F_TILE), F_TILE)
                acc = jnp.dot(rows[k], win_buf[slot, :, cols], preferred_element_type=jnp.float32)
                hidden[:rows_all, cols] = jnp.maximum(acc, 0.0).astype(jnp.bfloat16)
                acc = jnp.dot(spill_in[...], win_buf[slot, :, cols], preferred_element_type=jnp.float32)
                hidden[rows_all:, cols] = jnp.maximum(acc, 0.0).astype(jnp.bfloat16)
                return c

            lax.fori_loop(0, hidden_dim // F_TILE, first, 0)

            def second(n, c):
                cols = pl.ds(pl.multiple_of(n * N_TILE, N_TILE), N_TILE)
                acc = jnp.dot(hidden[:rows_all], wout_buf[slot, :, cols], preferred_element_type=jnp.float32)
                rows[k, :, cols] = acc.astype(jnp.bfloat16)
                acc = jnp.dot(hidden[rows_all:], wout_buf[slot, :, cols], preferred_element_type=jnp.float32)
                mine = spill_expert[:, :1] == k.astype(jnp.float32)
                spill_out[:, cols] = jnp.where(mine, acc, spill_out[:, cols].astype(jnp.float32)).astype(jnp.bfloat16)
                return c

            lax.fori_loop(0, model_dim // N_TILE, second, 0)
            for dist in peers:
                back_copy(k, dist).start()
            own_back(k).start()
            return carry

        lax.fori_loop(0, local_experts, expert, 0)
        for dist in peers:
            spill_back(dist).start()
        own_spill_back().start()

    pl.run_scoped(
        expert_phase,
        pltpu.VMEM((2, model_dim, hidden_dim), jnp.bfloat16),
        pltpu.VMEM((2, hidden_dim, model_dim), jnp.bfloat16),
        pltpu.VMEM((rows_all + spill_all, hidden_dim), jnp.bfloat16),
    )

    def gate_phase(tile_ref):
        tok_copy(0, 0, tile_ref).start()
        expert_ids = lax.broadcasted_iota(jnp.int32, (num_experts, TOK_TILE), 0)

        def gate_tile(i, carry):
            slot = lax.rem(i, 2)

            @pl.when(i + 1 < tok_tiles)
            def _():
                tok_copy(i + 1, 1 - slot, tile_ref).start()

            tok_copy(i, slot, tile_ref).wait()
            tile = tile_ref[slot]
            part = [jnp.dot(tile, w_router[p], preferred_element_type=jnp.float32) for p in range(3)]
            logits = jnp.transpose(part[0] + (part[1] + part[2]))[:num_experts]
            weight = jnp.exp(logits - jnp.max(logits, axis=0, keepdims=True))
            own = jnp.sum(jnp.where(expert_ids == choice[i], weight, 0.0), axis=0, keepdims=True)
            gate_ref[i] = own / jnp.sum(weight, axis=0, keepdims=True)
            return carry

        lax.fori_loop(0, tok_tiles, gate_tile, 0)

    pl.run_scoped(gate_phase, pltpu.VMEM((2, TOK_TILE, model_dim), jnp.bfloat16))

    def finish(k, carry):
        for dist in peers:
            out_copy(k, dist).wait_send()
        for dist in peers:
            back_copy(k, dist).wait()
        own_back(k).wait()
        return carry

    lax.fori_loop(0, local_experts, finish, 0)
    for dist in peers:
        ids_copy(dist).wait_send()
        spill_copy(dist).wait_send()
        spill_back(dist).wait()
    own_spill_back().wait()


def split_router(w_router):
    pad = -w_router.shape[1] % LANES
    rest = jnp.pad(w_router, ((0, 0), (0, pad)))
    parts = []
    for _ in range(3):
        piece = lax.reduce_precision(rest, 8, 7)
        parts.append(piece.astype(jnp.bfloat16))
        rest = rest - piece
    return jnp.stack(parts)


def exchange(groups, cap, spill, holder, tokens, ids, choice, w_router, w_in, w_out):
    local_experts, model_dim, hidden_dim = w_in.shape
    num_experts = groups * local_experts
    tok_count = tokens.shape[0]
    tok_tiles = tok_count // TOK_TILE
    hbm = pl.BlockSpec(memory_space=pl.ANY)
    vmem = pl.BlockSpec(memory_space=pltpu.VMEM)
    per_block = pltpu.SemaphoreType.DMA((groups, local_experts + 1))
    own = pltpu.SemaphoreType.DMA((local_experts + 1,))
    return pl.pallas_call(
        functools.partial(exchange_kernel, groups, num_experts, cap, spill),
        out_shape=(
            jax.ShapeDtypeStruct((num_experts * cap + groups * spill, model_dim), jnp.bfloat16),
            jax.ShapeDtypeStruct((tok_tiles, 1, TOK_TILE), jnp.float32),
            jax.ShapeDtypeStruct((groups, 8, LANES), jnp.float32),
            jax.ShapeDtypeStruct((local_experts, groups * cap, model_dim), jnp.bfloat16),
            jax.ShapeDtypeStruct((groups * spill, model_dim), jnp.bfloat16),
        ),
        in_specs=[pl.BlockSpec(memory_space=pltpu.SMEM), hbm, vmem, vmem, vmem, hbm, hbm],
        out_specs=(hbm, vmem, vmem, hbm, hbm),
        scratch_shapes=[
            pltpu.VMEM((local_experts, groups * cap, model_dim), jnp.bfloat16),
            pltpu.VMEM((groups * spill, model_dim), jnp.bfloat16),
            pltpu.VMEM((groups * spill, model_dim), jnp.bfloat16),
            pltpu.VMEM((groups * spill, LANES), jnp.float32),
            per_block,
            per_block,
            per_block,
            per_block,
            own,
            own,
            pltpu.SemaphoreType.DMA((groups,)),
            pltpu.SemaphoreType.DMA((groups,)),
            pltpu.SemaphoreType.DMA((2, 2)),
            pltpu.SemaphoreType.DMA((4,)),
            pltpu.SemaphoreType.DMA((2,)),
        ],
        compiler_params=pltpu.CompilerParams(collective_id=0, has_side_effects=True, vmem_limit_bytes=VMEM_LIMIT),
        name="exchange",
    )(holder.reshape(-1), tokens, ids, choice.reshape(tok_tiles, 1, TOK_TILE), split_router(w_router), w_in, w_out)


def combine_kernel(in_tile, slot_ref, gate_ref, keep_ref, src_hbm, y_ref, src_lin, stage, picked, sems):
    i = pl.program_id(0)
    tile, model_dim = y_ref.shape
    pieces = model_dim // LANES
    in_tiles = src_hbm.shape[0] // in_tile
    depth = stage.shape[0]

    @pl.when(i == 0)
    def _():
        def copy(b):
            slot = lax.rem(b, depth)
            return pltpu.make_async_copy(src_hbm.at[pl.ds(pl.multiple_of(b * in_tile, in_tile), in_tile)], stage.at[slot], sems.at[slot])

        for b in range(depth - 1):
            copy(jnp.int32(b)).start()

        def load(b, carry):
            @pl.when(b + depth - 1 < in_tiles)
            def _():
                copy(b + depth - 1).start()

            copy(b).wait()
            for j in range(pieces):
                src_lin[pl.ds(b * (in_tile * pieces) + j, in_tile, stride=pieces), :] = stage[lax.rem(b, depth), :, j * LANES:(j + 1) * LANES].astype(jnp.float32)
            return carry

        lax.fori_loop(0, in_tiles, load, 0)

    def pick(q, carry):
        for u in range(UNROLL):
            at = q * UNROLL + u
            row = slot_ref[i * tile + at]
            picked[pl.ds(at * pieces, pieces), :] = src_lin[pl.ds(row * pieces, pieces), :]
        return carry

    lax.fori_loop(0, tile // UNROLL, pick, 0)
    gate_row = jnp.where(keep_ref[0] > 0.0, gate_ref[0], -1.0)
    gate = jnp.transpose(jnp.broadcast_to(gate_row, (8, tile)))[:, :1]
    for j in range(pieces):
        value = picked[pl.ds(j, tile, stride=pieces), :] * gate
        y_ref[:, j * LANES:(j + 1) * LANES] = jnp.where(gate >= 0.0, value, 0.0).astype(jnp.bfloat16)


def combine(flat_out, slot_index, gate, keep):
    row_count, model_dim = flat_out.shape
    tok_tiles, _, tile = gate.shape
    pieces = model_dim // LANES
    in_tile = max(n for n in range(16, 513, 16) if row_count % n == 0)
    row_spec = pl.BlockSpec((1, 1, tile), lambda i, s: (i, 0, 0))
    return pl.pallas_call(
        functools.partial(combine_kernel, in_tile),
        grid_spec=pltpu.PrefetchScalarGridSpec(
            num_scalar_prefetch=1,
            grid=(tok_tiles,),
            in_specs=[row_spec, row_spec, pl.BlockSpec(memory_space=pl.ANY)],
            out_specs=pl.BlockSpec((tile, model_dim), lambda i, s: (i, 0)),
            scratch_shapes=[
                pltpu.VMEM((row_count * pieces, LANES), jnp.float32),
                pltpu.VMEM((4, in_tile, model_dim), jnp.bfloat16),
                pltpu.VMEM((tile * pieces, LANES), jnp.float32),
                pltpu.SemaphoreType.DMA((4,)),
            ],
        ),
        out_shape=jax.ShapeDtypeStruct((tok_tiles * tile, model_dim), jnp.bfloat16),
        compiler_params=pltpu.CompilerParams(vmem_limit_bytes=VMEM_LIMIT),
        name="combine",
    )(slot_index.reshape(-1), gate, keep.reshape(gate.shape), flat_out)


def full_capacity(groups, capacity, tokens, full_slot, gate, keep, w_in, w_out):
    tok_count, model_dim = tokens.shape
    local_experts = w_in.shape[0]
    slots = local_experts * groups * capacity
    slot_index = full_slot.reshape(-1)
    holder = jnp.full((slots + 1,), tok_count, jnp.int32).at[slot_index].set(jnp.arange(tok_count, dtype=jnp.int32))
    buffer = jnp.take(tokens, holder[:-1], axis=0, mode="fill", fill_value=0)
    recv_buf = lax.all_to_all(buffer.reshape(groups, local_experts, capacity, model_dim), "ep", 0, 0, tiled=True)

    def one_expert(operands):
        rows_of, first, second = operands
        hidden_act = jax.nn.relu(jnp.dot(rows_of.reshape(groups * capacity, model_dim), first, preferred_element_type=jnp.float32)).astype(jnp.bfloat16)
        return jnp.dot(hidden_act, second, preferred_element_type=jnp.float32).astype(jnp.bfloat16).reshape(groups, capacity, model_dim)

    expert_rows = lax.map(one_expert, (jnp.swapaxes(recv_buf, 0, 1), w_in, w_out))
    back_buf = lax.all_to_all(jnp.swapaxes(expert_rows, 0, 1), "ep", 0, 0, tiled=True)
    return combine(back_buf.reshape(slots, model_dim), jnp.minimum(slot_index, slots - 1), gate, keep)


def solution(mesh):
    groups = mesh.shape["ep"]

    def local_block(tokens, expert_idx, w_router, w_in, w_out):
        tok_count = tokens.shape[0]
        num_experts = w_in.shape[0] * groups
        capacity = (5 * tok_count + 4 * num_experts - 1) // (4 * num_experts)
        main = tok_count // num_experts
        spill = capacity // 2
        holder, ids, slot_index, full_slot, keep = route(expert_idx, groups, num_experts, capacity, main, spill)
        back_buf, gate, ids_in, _, _ = exchange(groups, main, spill, holder, tokens, ids, expert_idx, w_router, w_in, w_out)
        too_many = jnp.max(ids_in[:, 0, LANES - 1]) > 0.0
        return lax.cond(
            too_many,
            lambda: full_capacity(groups, capacity, tokens, full_slot, gate, keep, w_in, w_out),
            lambda: combine(back_buf, slot_index, gate, keep))

    return jax.shard_map(local_block, mesh=mesh, in_specs=(P(("dp", "ep"), None), P(("dp", "ep")), P(None, None), P("ep", None, None), P("ep", None, None)), out_specs=P(("dp", "ep"), None), check_vma=False)
```

```python
import functools

import jax
import jax.numpy as jnp
from jax import lax
from jax.experimental import pallas as pl
from jax.experimental.pallas import tpu as pltpu
from jax.sharding import PartitionSpec as P

MESH = pl.DeviceIdType.MESH
LANES = 128
F_TILE = 512
N_TILE = 256
ROUTE_CHUNK = 256
TOK_TILE = 512
PICK_UNROLL = 64
UNROLL = 16
VMEM_LIMIT = 62 * 1024 * 1024


def route_kernel(groups, num_experts, capacity, main, spill, pieces, choice_ref, holder_ref, ids_ref, slot_ref, full_ref, kept_ref):
    parts, _, chunk = choice_ref.shape
    local_experts = num_experts // groups
    table_rows = num_experts + groups
    expert_ids = lax.broadcasted_iota(jnp.int32, (num_experts, chunk), 0)
    row_ids = lax.broadcasted_iota(jnp.int32, (table_rows, chunk), 0)
    col_ids = lax.broadcasted_iota(jnp.int32, (LANES, chunk), 0)
    local_id = lax.broadcasted_iota(jnp.int32, (table_rows, chunk), 1).astype(jnp.float32)
    upper = (lax.broadcasted_iota(jnp.int32, (chunk, chunk), 0) <= lax.broadcasted_iota(jnp.int32, (chunk, chunk), 1)).astype(jnp.bfloat16)

    def count(c, acc):
        return acc + (expert_ids == choice_ref[c]).astype(jnp.float32)

    totals = jnp.sum(lax.fori_loop(0, parts, count, jnp.zeros((num_experts, chunk), jnp.float32), unroll=4), axis=1, keepdims=True)
    extra = jnp.clip(totals - main, 0.0, float(capacity - main))
    row = lax.broadcasted_iota(jnp.int32, (num_experts, num_experts), 0)
    col = lax.broadcasted_iota(jnp.int32, (num_experts, num_experts), 1)
    same = col < row
    for j in range(1, groups):
        same = same & ((row >= j * local_experts) == (col >= j * local_experts))
    offset = jnp.dot(same.astype(jnp.bfloat16), jnp.broadcast_to(extra, (num_experts, LANES)).astype(jnp.bfloat16), preferred_element_type=jnp.float32)[:, :1]
    too_many = jnp.max(offset + extra, axis=0, keepdims=True) > spill
    scale = 2.0 * parts * chunk

    def body(c, carry):
        before, table, ids = carry
        choice = choice_ref[c]
        ones = (expert_ids == choice).astype(jnp.float32)
        running = jnp.dot(ones.astype(jnp.bfloat16), upper, preferred_element_type=jnp.float32) + before
        packed = jnp.sum(ones * (running + (offset * scale - 1.0)), axis=0, keepdims=True).astype(jnp.int32)
        position = packed & (int(scale) - 1)
        start = (packed - position).astype(jnp.float32) * (1.0 / scale)
        dest = jnp.zeros_like(choice)
        for j in range(1, groups):
            dest = dest + (choice >= j * local_experts).astype(jnp.int32)
        kept = position < capacity
        is_main = position < main
        spill_at = start.astype(jnp.int32) + position - main
        table_row = jnp.where(is_main, choice, jnp.where(kept, num_experts + dest, table_rows))
        table_col = jnp.where(is_main, position, spill_at)
        slot_ref[c] = pieces * jnp.where(is_main, choice * main + position, jnp.where(kept, num_experts * main + dest * spill + jnp.minimum(spill_at, spill - 1), 0))
        full_ref[c] = jnp.where(kept, choice * capacity + position, num_experts * capacity)
        kept_ref[c] = jnp.where(kept, choice, -1).astype(jnp.float32)
        at_row = (row_ids == table_row).astype(jnp.float32)
        at_col = (col_ids == table_col).astype(jnp.float32).astype(jnp.bfloat16)
        local_expert = (choice - dest * local_experts).astype(jnp.float32)
        stacked = jnp.concatenate([at_row * local_id, at_row, at_row[num_experts:] * local_expert], axis=0).astype(jnp.bfloat16)
        found = lax.dot_general(stacked, at_col, (((1,), (1,)), ((), ())), preferred_element_type=jnp.float32)
        table = table + found[:table_rows] + found[table_rows:2 * table_rows] * (c * chunk).astype(jnp.float32)
        return running[:, chunk - 1:], table, ids + found[2 * table_rows:]

    init = (jnp.zeros((num_experts, 1), jnp.float32), jnp.zeros((table_rows, LANES), jnp.float32), jnp.zeros((groups, LANES), jnp.float32))
    _, table, ids = lax.fori_loop(0, parts, body, init, unroll=4)
    holder_ref[...] = pieces * table.astype(jnp.int32)
    last = lax.broadcasted_iota(jnp.int32, (groups, LANES), 1) == LANES - 1
    ids = jnp.where(last, too_many.astype(jnp.float32), ids)
    for j in range(groups):
        ids_ref[j] = jnp.broadcast_to(ids[j:j + 1], (8, LANES))


def route(expert_idx, groups, num_experts, capacity, main, spill, pieces):
    tok_count = expert_idx.shape[0]
    parts = tok_count // ROUTE_CHUNK
    shape = (parts, 1, ROUTE_CHUNK)
    return pl.pallas_call(
        functools.partial(route_kernel, groups, num_experts, capacity, main, spill, pieces),
        out_shape=(
            jax.ShapeDtypeStruct((num_experts + groups, LANES), jnp.int32),
            jax.ShapeDtypeStruct((groups, 8, LANES), jnp.float32),
            jax.ShapeDtypeStruct(shape, jnp.int32),
            jax.ShapeDtypeStruct(shape, jnp.int32),
            jax.ShapeDtypeStruct(shape, jnp.float32),
        ),
        name="route",
    )(expert_idx.reshape(shape))


def exchange_kernel(groups, num_experts, cap, spill, holder, tokens, ids, kept, w_router, w_in, w_out,
                    back_buf, gate_ref, ids_in, send_buf, send_spill,
                    rows, spill_in, spill_out, spill_expert, dsend, drecv, rsend, rrecv, own_in, own_out, isend, irecv, wsem, tok_sem, stage_sem):
    me = lax.axis_index("ep")
    local_experts, model_dim, hidden_dim = w_in.shape
    width = LANES
    tok_count = tokens.shape[0]
    tok_tiles = tok_count // TOK_TILE
    pieces = model_dim // LANES
    peers = tuple(range(1, groups))
    rows_all = groups * cap
    spill_all = groups * spill
    last = local_experts

    barrier = pltpu.get_barrier_semaphore()
    for dist in peers:
        pl.semaphore_signal(barrier, inc=1, device_id={"ep": lax.rem(me + dist, groups)}, device_id_type=MESH)

    def block(i):
        return pl.ds(pl.multiple_of(i * cap, cap), cap)

    def spill_block(i):
        return pl.ds(pl.multiple_of(i * spill, spill), spill)

    def back_block(k):
        return pl.ds(pl.multiple_of((me * local_experts + k) * cap, cap), cap)

    def back_spill(i):
        return pl.ds(pl.multiple_of(num_experts * cap + i * spill, 16), spill)

    def spill_copy(dist):
        to = lax.rem(me + dist, groups)
        return pltpu.make_async_remote_copy(
            src_ref=send_spill.at[spill_block(to)], dst_ref=spill_in.at[spill_block(me)],
            send_sem=dsend.at[dist, last], recv_sem=drecv.at[dist, last], device_id={"ep": to}, device_id_type=MESH)

    def own_spill():
        return pltpu.make_async_copy(send_spill.at[spill_block(me)], spill_in.at[spill_block(me)], own_in.at[last])

    def ids_copy(dist):
        to = lax.rem(me + dist, groups)
        return pltpu.make_async_remote_copy(
            src_ref=ids.at[to], dst_ref=ids_in.at[me],
            send_sem=isend.at[dist], recv_sem=irecv.at[dist], device_id={"ep": to}, device_id_type=MESH)

    def own_ids():
        return pltpu.make_async_copy(ids.at[me], ids_in.at[me], isend.at[0])

    def spill_back(dist):
        to = lax.rem(me + dist, groups)
        return pltpu.make_async_remote_copy(
            src_ref=spill_out.at[spill_block(to)], dst_ref=back_buf.at[back_spill(me)],
            send_sem=rsend.at[dist, last], recv_sem=rrecv.at[dist, last], device_id={"ep": to}, device_id_type=MESH)

    def own_spill_back():
        return pltpu.make_async_copy(spill_out.at[spill_block(me)], back_buf.at[back_spill(me)], own_out.at[last])

    def out_copy(k, dist):
        to = lax.rem(me + dist, groups)
        return pltpu.make_async_remote_copy(
            src_ref=send_buf.at[k, block(to)], dst_ref=rows.at[k, block(me)],
            send_sem=dsend.at[dist, k], recv_sem=drecv.at[dist, k], device_id={"ep": to}, device_id_type=MESH)

    def own_copy(k):
        return pltpu.make_async_copy(send_buf.at[k, block(me)], rows.at[k, block(me)], own_in.at[k])

    def back_copy(k, dist):
        to = lax.rem(me + dist, groups)
        return pltpu.make_async_remote_copy(
            src_ref=rows.at[k, block(to)], dst_ref=back_buf.at[back_block(k)],
            send_sem=rsend.at[dist, k], recv_sem=rrecv.at[dist, k], device_id={"ep": to}, device_id_type=MESH)

    def own_back(k):
        return pltpu.make_async_copy(rows.at[k, block(me)], back_buf.at[back_block(k)], own_out.at[k])

    def tok_copy(i, slot, tile_ref):
        return pltpu.make_async_copy(tokens.at[pl.ds(pl.multiple_of(i * TOK_TILE, TOK_TILE), TOK_TILE)], tile_ref.at[slot], tok_sem.at[slot])

    def send_phase(tok_lin, tile_ref, picked, packed):
        depth = tile_ref.shape[0]
        for i in range(depth):
            tok_copy(i, i, tile_ref).start()

        def load_tile(i, carry):
            slot = lax.rem(i, depth)
            tok_copy(i, slot, tile_ref).wait()
            for j in range(pieces):
                tok_lin[pl.ds(i * (TOK_TILE * pieces) + j, TOK_TILE, stride=pieces), :] = tile_ref[slot, :, j * LANES:(j + 1) * LANES].astype(jnp.float32)

            @pl.when(i + depth < tok_tiles)
            def _():
                tok_copy(i + depth, slot, tile_ref).start()

            return carry

        lax.fori_loop(0, tok_tiles, load_tile, 0)
        pl.semaphore_wait(barrier, groups - 1)
        for dist in peers:
            ids_copy(dist).start()
        own_ids().start()

        def pick(first_slot, first_row, n):
            def some(q, c):
                for u in range(UNROLL):
                    at = q * UNROLL + u
                    tok = holder[first_slot + at]
                    picked[pl.ds((first_row + at) * pieces, pieces), :] = tok_lin[pl.ds(tok, pieces), :]
                return c

            lax.fori_loop(0, n // UNROLL, some, 0)

        def spill_dest(j, c):
            pick((num_experts + j) * width, j * spill, spill)
            return c

        lax.fori_loop(0, groups, spill_dest, 0)
        for j in range(pieces):
            packed[1, :spill_all, j * LANES:(j + 1) * LANES] = picked[pl.ds(j, spill_all, stride=pieces), :].astype(jnp.bfloat16)
        spill_stage = pltpu.make_async_copy(packed.at[1, pl.ds(0, spill_all)], send_spill, stage_sem.at[1])
        spill_stage.start()

        def stage_copy(k):
            slot = lax.rem(k, 2)
            return pltpu.make_async_copy(packed.at[slot], send_buf.at[k], stage_sem.at[slot])

        def send(k):
            stage_copy(k).wait()
            for dist in peers:
                out_copy(k, dist).start()
            own_copy(k).start()

        def gather(k, carry):
            def one_dest(j, c):
                pick((j * local_experts + k) * width, j * cap, cap)
                return c

            lax.fori_loop(0, groups, one_dest, 0)
            slot = lax.rem(k, 2)
            for j in range(pieces):
                packed[slot, :, j * LANES:(j + 1) * LANES] = picked[pl.ds(j, rows_all, stride=pieces), :].astype(jnp.bfloat16)

            @pl.when(k > 0)
            def _():
                send(k - 1)

            @pl.when(k == 0)
            def _():
                spill_stage.wait()
                for dist in peers:
                    spill_copy(dist).start()
                own_spill().start()

            stage_copy(k).start()
            return carry

        lax.fori_loop(0, local_experts, gather, 0)
        send(local_experts - 1)

    pl.run_scoped(
        send_phase,
        pltpu.VMEM((tok_count * pieces, LANES), jnp.float32),
        pltpu.VMEM((8, TOK_TILE, model_dim), jnp.bfloat16),
        pltpu.VMEM((rows_all * pieces, LANES), jnp.float32),
        pltpu.VMEM((2, rows_all, model_dim), jnp.bfloat16),
    )

    def expert_phase(win_buf, wout_buf, hidden):
        def weights(k, slot):
            return (pltpu.make_async_copy(w_in.at[k], win_buf.at[slot], wsem.at[0, slot]),
                    pltpu.make_async_copy(w_out.at[k], wout_buf.at[slot], wsem.at[1, slot]))

        for cp in weights(0, 0):
            cp.start()
        own_ids().wait()
        own_spill().wait()
        for dist in peers:
            ids_copy(dist).wait_recv()
            spill_copy(dist).wait_recv()
        for j in range(groups):
            column = jnp.transpose(ids_in[j])[:spill, :1]
            spill_expert[spill_block(j), :] = jnp.broadcast_to(column, (spill, LANES))
        spill_out[...] = jnp.zeros_like(spill_out)

        def expert(k, carry):
            slot = lax.rem(k, 2)

            @pl.when(k + 1 < local_experts)
            def _():
                for cp in weights(k + 1, 1 - slot):
                    cp.start()

            for dist in peers:
                out_copy(k, dist).wait_recv()
            own_copy(k).wait()
            for cp in weights(k, slot):
                cp.wait()

            def first(f, c):
                cols = pl.ds(pl.multiple_of(f * F_TILE, F_TILE), F_TILE)
                acc = jnp.dot(rows[k], win_buf[slot, :, cols], preferred_element_type=jnp.float32)
                hidden[:rows_all, cols] = jnp.maximum(acc, 0.0).astype(jnp.bfloat16)
                acc = jnp.dot(spill_in[...], win_buf[slot, :, cols], preferred_element_type=jnp.float32)
                hidden[rows_all:, cols] = jnp.maximum(acc, 0.0).astype(jnp.bfloat16)
                return c

            lax.fori_loop(0, hidden_dim // F_TILE, first, 0)

            def second(n, c):
                cols = pl.ds(pl.multiple_of(n * N_TILE, N_TILE), N_TILE)
                acc = jnp.dot(hidden[:rows_all], wout_buf[slot, :, cols], preferred_element_type=jnp.float32)
                rows[k, :, cols] = acc.astype(jnp.bfloat16)
                acc = jnp.dot(hidden[rows_all:], wout_buf[slot, :, cols], preferred_element_type=jnp.float32)
                mine = spill_expert[:, :1] == k.astype(jnp.float32)
                spill_out[:, cols] = jnp.where(mine, acc, spill_out[:, cols].astype(jnp.float32)).astype(jnp.bfloat16)
                return c

            lax.fori_loop(0, model_dim // N_TILE, second, 0)
            for dist in peers:
                back_copy(k, dist).start()
            own_back(k).start()
            return carry

        lax.fori_loop(0, local_experts, expert, 0)
        for dist in peers:
            spill_back(dist).start()
        own_spill_back().start()

    pl.run_scoped(
        expert_phase,
        pltpu.VMEM((2, model_dim, hidden_dim), jnp.bfloat16),
        pltpu.VMEM((2, hidden_dim, model_dim), jnp.bfloat16),
        pltpu.VMEM((rows_all + spill_all, hidden_dim), jnp.bfloat16),
    )

    def gate_phase(tile_ref, gate_tile_ref):
        tok_copy(0, 0, tile_ref).start()
        lane = lax.broadcasted_iota(jnp.int32, (TOK_TILE, w_router.shape[2]), 1)

        def gate_copy(i, slot):
            return pltpu.make_async_copy(gate_tile_ref.at[slot], gate_ref.at[pl.ds(pl.multiple_of(i * TOK_TILE, TOK_TILE), TOK_TILE)], stage_sem.at[slot])

        def gate_tile(i, carry):
            slot = lax.rem(i, 2)

            @pl.when(i + 1 < tok_tiles)
            def _():
                tok_copy(i + 1, 1 - slot, tile_ref).start()

            tok_copy(i, slot, tile_ref).wait()
            tile = tile_ref[slot]
            part = [jnp.dot(tile, w_router[p], preferred_element_type=jnp.float32) for p in range(3)]
            logits = jnp.where(lane < num_experts, part[0] + (part[1] + part[2]), -jnp.inf)
            weight = jnp.exp(logits - jnp.max(logits, axis=1, keepdims=True))
            expert_of = jnp.transpose(jnp.broadcast_to(kept[i], (8, TOK_TILE)))[:, :1]
            own = jnp.sum(jnp.where(lane.astype(jnp.float32) == expert_of, weight, 0.0), axis=1, keepdims=True)
            gate = jnp.where(expert_of >= 0.0, own / jnp.sum(weight, axis=1, keepdims=True), -1.0)

            @pl.when(i >= 2)
            def _():
                gate_copy(i - 2, slot).wait()

            gate_tile_ref[slot] = jnp.broadcast_to(gate, (TOK_TILE, LANES))
            gate_copy(i, slot).start()
            return carry

        lax.fori_loop(0, tok_tiles, gate_tile, 0)
        for i in range(tok_tiles - 2, tok_tiles):
            gate_copy(i, i % 2).wait()

    pl.run_scoped(gate_phase, pltpu.VMEM((2, TOK_TILE, model_dim), jnp.bfloat16), pltpu.VMEM((2, TOK_TILE, LANES), jnp.float32))

    def finish(k, carry):
        for dist in peers:
            out_copy(k, dist).wait_send()
        for dist in peers:
            back_copy(k, dist).wait()
        own_back(k).wait()
        return carry

    lax.fori_loop(0, local_experts, finish, 0)
    for dist in peers:
        ids_copy(dist).wait_send()
        spill_copy(dist).wait_send()
        spill_back(dist).wait()
    own_spill_back().wait()


def split_router(w_router):
    pad = -w_router.shape[1] % LANES
    rest = jnp.pad(w_router, ((0, 0), (0, pad)))
    parts = []
    for _ in range(3):
        piece = lax.reduce_precision(rest, 8, 7)
        parts.append(piece.astype(jnp.bfloat16))
        rest = rest - piece
    return jnp.stack(parts)


def exchange(groups, cap, spill, holder, tokens, ids, kept, w_router, w_in, w_out):
    local_experts, model_dim, hidden_dim = w_in.shape
    num_experts = groups * local_experts
    tok_count = tokens.shape[0]
    tok_tiles = tok_count // TOK_TILE
    hbm = pl.BlockSpec(memory_space=pl.ANY)
    vmem = pl.BlockSpec(memory_space=pltpu.VMEM)
    per_block = pltpu.SemaphoreType.DMA((groups, local_experts + 1))
    own = pltpu.SemaphoreType.DMA((local_experts + 1,))
    return pl.pallas_call(
        functools.partial(exchange_kernel, groups, num_experts, cap, spill),
        out_shape=(
            jax.ShapeDtypeStruct((num_experts * cap + groups * spill, model_dim), jnp.bfloat16),
            jax.ShapeDtypeStruct((tok_count, LANES), jnp.float32),
            jax.ShapeDtypeStruct((groups, 8, LANES), jnp.float32),
            jax.ShapeDtypeStruct((local_experts, groups * cap, model_dim), jnp.bfloat16),
            jax.ShapeDtypeStruct((groups * spill, model_dim), jnp.bfloat16),
        ),
        in_specs=[pl.BlockSpec(memory_space=pltpu.SMEM), hbm, vmem, vmem, vmem, hbm, hbm],
        out_specs=(hbm, hbm, vmem, hbm, hbm),
        scratch_shapes=[
            pltpu.VMEM((local_experts, groups * cap, model_dim), jnp.bfloat16),
            pltpu.VMEM((groups * spill, model_dim), jnp.bfloat16),
            pltpu.VMEM((groups * spill, model_dim), jnp.bfloat16),
            pltpu.VMEM((groups * spill, LANES), jnp.float32),
            per_block,
            per_block,
            per_block,
            per_block,
            own,
            own,
            pltpu.SemaphoreType.DMA((groups,)),
            pltpu.SemaphoreType.DMA((groups,)),
            pltpu.SemaphoreType.DMA((2, 2)),
            pltpu.SemaphoreType.DMA((8,)),
            pltpu.SemaphoreType.DMA((2,)),
        ],
        compiler_params=pltpu.CompilerParams(collective_id=0, has_side_effects=True, vmem_limit_bytes=VMEM_LIMIT),
        name="exchange",
    )(holder.reshape(-1), tokens, ids, kept.reshape(tok_tiles, 1, TOK_TILE), split_router(w_router), w_in, w_out)


def combine_kernel(in_tile, slot_ref, gate_hbm, src_hbm, y_hbm, src_lin, stage, gates, picked, out_tile, in_sem, gate_sem, out_sem):
    tok_tiles, tile, _ = gates.shape
    model_dim = src_hbm.shape[1]
    pieces = model_dim // LANES
    in_tiles = src_hbm.shape[0] // in_tile
    depth = stage.shape[0]
    out_depth = out_tile.shape[0]

    def load_copy(b):
        slot = lax.rem(b, depth)
        return pltpu.make_async_copy(src_hbm.at[pl.ds(pl.multiple_of(b * in_tile, in_tile), in_tile)], stage.at[slot], in_sem.at[slot])

    def store_copy(i):
        slot = lax.rem(i, out_depth)
        return pltpu.make_async_copy(out_tile.at[slot], y_hbm.at[pl.ds(pl.multiple_of(i * tile, tile), tile)], out_sem.at[slot])

    def start(b, carry):
        load_copy(b).start()
        return carry

    lax.fori_loop(0, min(depth, in_tiles), start, 0)

    def gate_copy(i):
        return pltpu.make_async_copy(gate_hbm.at[pl.ds(pl.multiple_of(i * tile, tile), tile)], gates.at[i], gate_sem.at[i])

    def load(b, carry):
        load_copy(b).wait()
        for j in range(pieces):
            src_lin[pl.ds(b * (in_tile * pieces) + j, in_tile, stride=pieces), :] = stage[lax.rem(b, depth), :, j * LANES:(j + 1) * LANES].astype(jnp.float32)

        @pl.when(b + depth < in_tiles)
        def _():
            load_copy(b + depth).start()

        return carry

    lax.fori_loop(0, in_tiles - depth, load, 0)

    def start_gate(i, carry):
        gate_copy(i).start()
        return carry

    lax.fori_loop(0, tok_tiles, start_gate, 0)
    lax.fori_loop(in_tiles - depth, in_tiles, load, 0)

    def emit(i, carry):
        def pick(q, c):
            for u in range(PICK_UNROLL):
                at = q * PICK_UNROLL + u
                row = slot_ref[i * tile + at]
                picked[pl.ds(at * pieces, pieces), :] = src_lin[pl.ds(row, pieces), :]
            return c

        lax.fori_loop(0, tile // PICK_UNROLL, pick, 0)
        gate_copy(i).wait()

        @pl.when(i >= out_depth)
        def _():
            store_copy(i - out_depth).wait()

        slot = lax.rem(i, out_depth)
        gate = gates[i]
        for j in range(pieces):
            value = picked[pl.ds(j, tile, stride=pieces), :] * gate
            out_tile[slot, :, j * LANES:(j + 1) * LANES] = jnp.where(gate >= 0.0, value, 0.0).astype(jnp.bfloat16)
        store_copy(i).start()
        return carry

    lax.fori_loop(0, tok_tiles, emit, 0)

    def drain(i, carry):
        store_copy(tok_tiles - out_depth + i).wait()
        return carry

    lax.fori_loop(0, out_depth, drain, 0)


def combine(flat_out, slot_index, gate):
    row_count, model_dim = flat_out.shape
    tile = TOK_TILE
    tok_tiles = gate.shape[0] // tile
    pieces = model_dim // LANES
    in_tile = max(n for n in range(16, 513, 16) if row_count % n == 0)
    depth = min(12, row_count // in_tile)
    out_depth = min(6, tok_tiles)
    hbm = pl.BlockSpec(memory_space=pl.ANY)
    return pl.pallas_call(
        functools.partial(combine_kernel, in_tile),
        in_specs=[pl.BlockSpec(memory_space=pltpu.SMEM), hbm, hbm],
        out_specs=hbm,
        scratch_shapes=[
            pltpu.VMEM((row_count * pieces, LANES), jnp.float32),
            pltpu.VMEM((depth, in_tile, model_dim), jnp.bfloat16),
            pltpu.VMEM((tok_tiles, tile, LANES), jnp.float32),
            pltpu.VMEM((tile * pieces, LANES), jnp.float32),
            pltpu.VMEM((out_depth, tile, model_dim), jnp.bfloat16),
            pltpu.SemaphoreType.DMA((depth,)),
            pltpu.SemaphoreType.DMA((tok_tiles,)),
            pltpu.SemaphoreType.DMA((out_depth,)),
        ],
        out_shape=jax.ShapeDtypeStruct((tok_tiles * tile, model_dim), jnp.bfloat16),
        compiler_params=pltpu.CompilerParams(vmem_limit_bytes=VMEM_LIMIT),
        name="combine",
    )(slot_index.reshape(-1), gate, flat_out)


def full_capacity(groups, capacity, tokens, full_slot, gate, w_in, w_out):
    tok_count, model_dim = tokens.shape
    local_experts = w_in.shape[0]
    slots = local_experts * groups * capacity
    slot_index = full_slot.reshape(-1)
    holder = jnp.full((slots + 1,), tok_count, jnp.int32).at[slot_index].set(jnp.arange(tok_count, dtype=jnp.int32))
    buffer = jnp.take(tokens, holder[:-1], axis=0, mode="fill", fill_value=0)
    recv_buf = lax.all_to_all(buffer.reshape(groups, local_experts, capacity, model_dim), "ep", 0, 0, tiled=True)

    def one_expert(operands):
        rows_of, first, second = operands
        hidden_act = jax.nn.relu(jnp.dot(rows_of.reshape(groups * capacity, model_dim), first, preferred_element_type=jnp.float32)).astype(jnp.bfloat16)
        return jnp.dot(hidden_act, second, preferred_element_type=jnp.float32).astype(jnp.bfloat16).reshape(groups, capacity, model_dim)

    expert_rows = lax.map(one_expert, (jnp.swapaxes(recv_buf, 0, 1), w_in, w_out))
    back_buf = lax.all_to_all(jnp.swapaxes(expert_rows, 0, 1), "ep", 0, 0, tiled=True)
    return combine(back_buf.reshape(slots, model_dim), jnp.minimum(slot_index, slots - 1) * (model_dim // LANES), gate)


def solution(mesh):
    groups = mesh.shape["ep"]

    def local_block(tokens, expert_idx, w_router, w_in, w_out):
        tok_count = tokens.shape[0]
        num_experts = w_in.shape[0] * groups
        capacity = (5 * tok_count + 4 * num_experts - 1) // (4 * num_experts)
        main = tok_count // num_experts
        spill = capacity // 2
        holder, ids, slot_index, full_slot, kept = route(expert_idx, groups, num_experts, capacity, main, spill, tokens.shape[1] // LANES)
        back_buf, gate, ids_in, _, _ = exchange(groups, main, spill, holder, tokens, ids, kept, w_router, w_in, w_out)
        too_many = jnp.max(ids_in[:, 0, LANES - 1]) > 0.0
        return lax.cond(
            too_many,
            lambda: full_capacity(groups, capacity, tokens, full_slot, gate, w_in, w_out),
            lambda: combine(back_buf, slot_index, gate))

    return jax.shard_map(local_block, mesh=mesh, in_specs=(P(("dp", "ep"), None), P(("dp", "ep")), P(None, None), P("ep", None, None), P("ep", None, None)), out_specs=P(("dp", "ep"), None), check_vma=False)
```

```python
import functools

import jax
import jax.numpy as jnp
from jax import lax
from jax.experimental import pallas as pl
from jax.experimental.pallas import tpu as pltpu
from jax.sharding import PartitionSpec as P

MESH = pl.DeviceIdType.MESH
LANES = 128
F_TILE = 512
N_TILE = 256
ROUTE_CHUNK = 256
TOK_TILE = 512
ROUTE_STEP = 2
PICK_UNROLL = 64
VMEM_LIMIT = 62 * 1024 * 1024


def route_tokens(groups, num_experts, capacity, main, spill, pieces, beside, choice_ref, holder_ref, ids_ref, slot_ref, full_ref, kept_ref):
    chunk = ROUTE_CHUNK
    per_tile = choice_ref.shape[2] // chunk
    parts = choice_ref.shape[0] * per_tile
    local_experts = num_experts // groups
    table_rows = num_experts + groups
    expert_ids = lax.broadcasted_iota(jnp.int32, (num_experts, chunk), 0)
    row_ids = lax.broadcasted_iota(jnp.int32, (table_rows, chunk), 0)
    col_ids = lax.broadcasted_iota(jnp.int32, (LANES, chunk), 0)
    local_id = lax.broadcasted_iota(jnp.int32, (table_rows, chunk), 1).astype(jnp.float32)
    upper = (lax.broadcasted_iota(jnp.int32, (chunk, chunk), 0) <= lax.broadcasted_iota(jnp.int32, (chunk, chunk), 1)).astype(jnp.bfloat16)

    def part_of(c):
        return c // per_tile, slice(None), pl.ds(pl.multiple_of(lax.rem(c, per_tile) * chunk, chunk), chunk)

    def count(c, acc):
        return acc + (expert_ids == choice_ref[part_of(c)]).astype(jnp.float32)

    totals = jnp.sum(lax.fori_loop(0, parts, count, jnp.zeros((num_experts, chunk), jnp.float32), unroll=4), axis=1, keepdims=True)
    extra = jnp.clip(totals - main, 0.0, float(capacity - main))
    row = lax.broadcasted_iota(jnp.int32, (num_experts, num_experts), 0)
    col = lax.broadcasted_iota(jnp.int32, (num_experts, num_experts), 1)
    same = col < row
    for j in range(1, groups):
        same = same & ((row >= j * local_experts) == (col >= j * local_experts))
    offset = jnp.dot(same.astype(jnp.bfloat16), jnp.broadcast_to(extra, (num_experts, LANES)).astype(jnp.bfloat16), preferred_element_type=jnp.float32)[:, :1]
    too_many = jnp.max(offset + extra, axis=0, keepdims=True) > spill
    scale = 2.0 * parts * chunk

    def body(c, carry):
        before, table, ids = carry
        choice = choice_ref[part_of(c)]
        ones = (expert_ids == choice).astype(jnp.float32)
        running = jnp.dot(ones.astype(jnp.bfloat16), upper, preferred_element_type=jnp.float32) + before
        packed = jnp.sum(ones * (running + (offset * scale - 1.0)), axis=0, keepdims=True).astype(jnp.int32)
        position = packed & (int(scale) - 1)
        start = (packed - position).astype(jnp.float32) * (1.0 / scale)
        dest = jnp.zeros_like(choice)
        for j in range(1, groups):
            dest = dest + (choice >= j * local_experts).astype(jnp.int32)
        kept = position < capacity
        is_main = position < main
        spill_at = start.astype(jnp.int32) + position - main
        table_row = jnp.where(is_main, choice, jnp.where(kept, num_experts + dest, table_rows))
        table_col = jnp.where(is_main, position, spill_at)
        slot_ref[part_of(c)] = pieces * jnp.where(is_main, choice * main + position, jnp.where(kept, num_experts * main + dest * spill + jnp.minimum(spill_at, spill - 1), 0))
        full_ref[part_of(c)] = jnp.where(kept, choice * capacity + position, num_experts * capacity)
        kept_ref[part_of(c)] = jnp.where(kept, choice, -1).astype(jnp.float32)
        at_row = (row_ids == table_row).astype(jnp.float32)
        at_col = (col_ids == table_col).astype(jnp.float32).astype(jnp.bfloat16)
        local_expert = (choice - dest * local_experts).astype(jnp.float32)
        stacked = jnp.concatenate([at_row * local_id, at_row, at_row[num_experts:] * local_expert], axis=0).astype(jnp.bfloat16)
        found = lax.dot_general(stacked, at_col, (((1,), (1,)), ((), ())), preferred_element_type=jnp.float32)
        table = table + found[:table_rows] + found[table_rows:2 * table_rows] * (c * chunk).astype(jnp.float32)
        return running[:, chunk - 1:], table, ids + found[2 * table_rows:]

    init = (jnp.zeros((num_experts, 1), jnp.float32), jnp.zeros((table_rows, LANES), jnp.float32), jnp.zeros((groups, LANES), jnp.float32))

    def several(i, carry):
        for u in range(ROUTE_STEP * per_tile):
            carry = body(i * (ROUTE_STEP * per_tile) + u, carry)
        return carry

    def with_tiles(i, carry):
        beside(i)
        return several(i, carry)

    _, table, ids = lax.fori_loop(0, parts // (ROUTE_STEP * per_tile), with_tiles, init)
    holder_ref[...] = pieces * jnp.clip(table.astype(jnp.int32), 0, parts * chunk - 1)
    last = lax.broadcasted_iota(jnp.int32, (groups, LANES), 1) == LANES - 1
    ids = jnp.where(last, too_many.astype(jnp.float32), ids)
    for j in range(groups):
        ids_ref[j] = jnp.broadcast_to(ids[j:j + 1], (8, LANES))


def exchange_kernel(groups, num_experts, capacity, cap, spill, tokens, choice, w_router, w_in, w_out,
                    back_buf, gate_ref, flag_ref, slot_ref, full_ref, send_buf, send_spill, ids,
                    rows, ids_in, table, ids_made, kept, holder, spill_in, spill_out, spill_expert, dsend, drecv, rsend, rrecv, own_in, own_out, isend, irecv, wsem, tok_sem, stage_sem, table_sem):
    me = lax.axis_index("ep")
    local_experts, model_dim, hidden_dim = w_in.shape
    tok_count = tokens.shape[0]
    tok_tiles = tok_count // TOK_TILE
    pieces = model_dim // LANES
    peers = tuple(range(1, groups))
    rows_all = groups * cap
    spill_all = groups * spill
    last = local_experts

    barrier = pltpu.get_barrier_semaphore()
    for dist in peers:
        pl.semaphore_signal(barrier, inc=1, device_id={"ep": lax.rem(me + dist, groups)}, device_id_type=MESH)

    def block(i):
        return pl.ds(pl.multiple_of(i * cap, cap), cap)

    def spill_block(i):
        return pl.ds(pl.multiple_of(i * spill, spill), spill)

    def back_block(k):
        return pl.ds(pl.multiple_of((me * local_experts + k) * cap, cap), cap)

    def back_spill(i):
        return pl.ds(pl.multiple_of(num_experts * cap + i * spill, 16), spill)

    def spill_copy(dist):
        to = lax.rem(me + dist, groups)
        return pltpu.make_async_remote_copy(
            src_ref=send_spill.at[spill_block(to)], dst_ref=spill_in.at[spill_block(me)],
            send_sem=dsend.at[dist, last], recv_sem=drecv.at[dist, last], device_id={"ep": to}, device_id_type=MESH)

    def own_spill():
        return pltpu.make_async_copy(send_spill.at[spill_block(me)], spill_in.at[spill_block(me)], own_in.at[last])

    def ids_copy(dist):
        to = lax.rem(me + dist, groups)
        return pltpu.make_async_remote_copy(
            src_ref=ids.at[to], dst_ref=ids_in.at[me],
            send_sem=isend.at[dist], recv_sem=irecv.at[dist], device_id={"ep": to}, device_id_type=MESH)

    def own_ids():
        return pltpu.make_async_copy(ids.at[me], ids_in.at[me], isend.at[0])

    def spill_back(dist):
        to = lax.rem(me + dist, groups)
        return pltpu.make_async_remote_copy(
            src_ref=spill_out.at[spill_block(to)], dst_ref=back_buf.at[back_spill(me)],
            send_sem=rsend.at[dist, last], recv_sem=rrecv.at[dist, last], device_id={"ep": to}, device_id_type=MESH)

    def own_spill_back():
        return pltpu.make_async_copy(spill_out.at[spill_block(me)], back_buf.at[back_spill(me)], own_out.at[last])

    def out_copy(k, dist):
        to = lax.rem(me + dist, groups)
        return pltpu.make_async_remote_copy(
            src_ref=send_buf.at[k, block(to)], dst_ref=rows.at[k, block(me)],
            send_sem=dsend.at[dist, k], recv_sem=drecv.at[dist, k], device_id={"ep": to}, device_id_type=MESH)

    def own_copy(k):
        return pltpu.make_async_copy(send_buf.at[k, block(me)], rows.at[k, block(me)], own_in.at[k])

    def back_copy(k, dist):
        to = lax.rem(me + dist, groups)
        return pltpu.make_async_remote_copy(
            src_ref=rows.at[k, block(to)], dst_ref=back_buf.at[back_block(k)],
            send_sem=rsend.at[dist, k], recv_sem=rrecv.at[dist, k], device_id={"ep": to}, device_id_type=MESH)

    def own_back(k):
        return pltpu.make_async_copy(rows.at[k, block(me)], back_buf.at[back_block(k)], own_out.at[k])

    def tok_copy(i, slot, tile_ref):
        return pltpu.make_async_copy(tokens.at[pl.ds(pl.multiple_of(i * TOK_TILE, TOK_TILE), TOK_TILE)], tile_ref.at[slot], tok_sem.at[slot])

    def send_phase(tok_lin, tile_ref, picked, packed):
        depth = tile_ref.shape[0]
        for i in range(depth):
            tok_copy(i, i, tile_ref).start()

        def load_tiles(step):
            for u in range(ROUTE_STEP):
                i = step * ROUTE_STEP + u
                tok_copy(i, lax.rem(i, depth), tile_ref).wait()
            for u in range(ROUTE_STEP):
                i = step * ROUTE_STEP + u
                for j in range(pieces):
                    tok_lin[pl.ds(i * (TOK_TILE * pieces) + j, TOK_TILE, stride=pieces), :] = tile_ref[lax.rem(i, depth), :, j * LANES:(j + 1) * LANES].astype(jnp.float32)

        route_tokens(groups, num_experts, capacity, cap, spill, pieces, load_tiles, choice, table, ids_made, slot_ref, full_ref, kept)
        table_copy = pltpu.make_async_copy(table, holder, table_sem.at[0])
        table_copy.start()
        ids_stage = pltpu.make_async_copy(ids_made, ids, table_sem.at[1])
        ids_stage.start()
        table_copy.wait()
        ids_stage.wait()
        pl.semaphore_wait(barrier, groups - 1)
        for dist in peers:
            ids_copy(dist).start()
        own_ids().start()

        def pick(table_row, first_row, n):
            for at in range(n):
                tok = holder[table_row, at]
                picked[pl.ds((first_row + at) * pieces, pieces), :] = tok_lin[pl.ds(tok, pieces), :]

        def spill_dest(j, c):
            pick(num_experts + j, j * spill, spill)
            return c

        lax.fori_loop(0, groups, spill_dest, 0)
        for j in range(pieces):
            packed[1, :spill_all, j * LANES:(j + 1) * LANES] = picked[pl.ds(j, spill_all, stride=pieces), :].astype(jnp.bfloat16)
        spill_stage = pltpu.make_async_copy(packed.at[1, pl.ds(0, spill_all)], send_spill, stage_sem.at[1])
        spill_stage.start()

        def stage_copy(k):
            slot = lax.rem(k, 2)
            return pltpu.make_async_copy(packed.at[slot], send_buf.at[k], stage_sem.at[slot])

        def send(k):
            stage_copy(k).wait()
            for dist in peers:
                out_copy(k, dist).start()
            own_copy(k).start()

        def gather(k, carry):
            def one_dest(j, c):
                pick(j * local_experts + k, j * cap, cap)
                return c

            lax.fori_loop(0, groups, one_dest, 0)
            slot = lax.rem(k, 2)
            for j in range(pieces):
                packed[slot, :, j * LANES:(j + 1) * LANES] = picked[pl.ds(j, rows_all, stride=pieces), :].astype(jnp.bfloat16)

            @pl.when(k > 0)
            def _():
                send(k - 1)

            @pl.when(k == 0)
            def _():
                spill_stage.wait()
                for dist in peers:
                    spill_copy(dist).start()
                own_spill().start()

            stage_copy(k).start()
            return carry

        lax.fori_loop(0, local_experts, gather, 0)
        send(local_experts - 1)

    pl.run_scoped(
        send_phase,
        pltpu.VMEM((tok_count * pieces, LANES), jnp.float32),
        pltpu.VMEM((tok_tiles, TOK_TILE, model_dim), jnp.bfloat16),
        pltpu.VMEM((rows_all * pieces, LANES), jnp.float32),
        pltpu.VMEM((2, rows_all, model_dim), jnp.bfloat16),
    )

    def expert_phase(win_buf, wout_buf, hidden):
        def weights(k, slot):
            return (pltpu.make_async_copy(w_in.at[k], win_buf.at[slot], wsem.at[0, slot]),
                    pltpu.make_async_copy(w_out.at[k], wout_buf.at[slot], wsem.at[1, slot]))

        for cp in weights(0, 0):
            cp.start()
        own_ids().wait()
        own_spill().wait()
        for dist in peers:
            ids_copy(dist).wait_recv()
            spill_copy(dist).wait_recv()
        for j in range(groups):
            column = jnp.transpose(ids_in[j])[:spill, :1]
            spill_expert[spill_block(j), :] = jnp.broadcast_to(column, (spill, LANES))
        spill_out[...] = jnp.zeros_like(spill_out)
        flag_ref[0] = jnp.max(ids_in[...][:, 0, LANES - 1:]).astype(jnp.int32)

        def expert(k, carry):
            slot = lax.rem(k, 2)

            @pl.when(k + 1 < local_experts)
            def _():
                for cp in weights(k + 1, 1 - slot):
                    cp.start()

            for dist in peers:
                out_copy(k, dist).wait_recv()
            own_copy(k).wait()
            for cp in weights(k, slot):
                cp.wait()

            def first(f, c):
                cols = pl.ds(pl.multiple_of(f * F_TILE, F_TILE), F_TILE)
                acc = jnp.dot(rows[k], win_buf[slot, :, cols], preferred_element_type=jnp.float32)
                hidden[:rows_all, cols] = jnp.maximum(acc, 0.0).astype(jnp.bfloat16)
                acc = jnp.dot(spill_in[...], win_buf[slot, :, cols], preferred_element_type=jnp.float32)
                hidden[rows_all:, cols] = jnp.maximum(acc, 0.0).astype(jnp.bfloat16)
                return c

            lax.fori_loop(0, hidden_dim // F_TILE, first, 0)

            def second(n, c):
                cols = pl.ds(pl.multiple_of(n * N_TILE, N_TILE), N_TILE)
                acc = jnp.dot(hidden[:rows_all], wout_buf[slot, :, cols], preferred_element_type=jnp.float32)
                rows[k, :, cols] = acc.astype(jnp.bfloat16)
                acc = jnp.dot(hidden[rows_all:], wout_buf[slot, :, cols], preferred_element_type=jnp.float32)
                mine = spill_expert[:, :1] == k.astype(jnp.float32)
                spill_out[:, cols] = jnp.where(mine, acc, spill_out[:, cols].astype(jnp.float32)).astype(jnp.bfloat16)
                return c

            lax.fori_loop(0, model_dim // N_TILE, second, 0)
            for dist in peers:
                back_copy(k, dist).start()
            own_back(k).start()
            return carry

        lax.fori_loop(0, local_experts, expert, 0)
        for dist in peers:
            spill_back(dist).start()
        own_spill_back().start()

    pl.run_scoped(
        expert_phase,
        pltpu.VMEM((2, model_dim, hidden_dim), jnp.bfloat16),
        pltpu.VMEM((2, hidden_dim, model_dim), jnp.bfloat16),
        pltpu.VMEM((rows_all + spill_all, hidden_dim), jnp.bfloat16),
    )

    def gate_phase(tile_ref, gate_tile_ref):
        tok_copy(0, 0, tile_ref).start()
        lane = lax.broadcasted_iota(jnp.int32, (TOK_TILE, w_router.shape[2]), 1)

        def gate_copy(i, slot):
            return pltpu.make_async_copy(gate_tile_ref.at[slot], gate_ref.at[pl.ds(pl.multiple_of(i * TOK_TILE, TOK_TILE), TOK_TILE)], stage_sem.at[slot])

        def gate_tile(i, carry):
            slot = lax.rem(i, 2)

            @pl.when(i + 1 < tok_tiles)
            def _():
                tok_copy(i + 1, 1 - slot, tile_ref).start()

            tok_copy(i, slot, tile_ref).wait()
            tile = tile_ref[slot]
            part = [jnp.dot(tile, w_router[p], preferred_element_type=jnp.float32) for p in range(3)]
            logits = jnp.where(lane < num_experts, part[0] + (part[1] + part[2]), -jnp.inf)
            weight = jnp.exp(logits - jnp.max(logits, axis=1, keepdims=True))
            expert_of = jnp.transpose(jnp.broadcast_to(kept[i], (8, TOK_TILE)))[:, :1]
            own = jnp.sum(jnp.where(lane.astype(jnp.float32) == expert_of, weight, 0.0), axis=1, keepdims=True)
            gate = jnp.where(expert_of >= 0.0, own / jnp.sum(weight, axis=1, keepdims=True), -1.0)

            @pl.when(i >= 2)
            def _():
                gate_copy(i - 2, slot).wait()

            gate_tile_ref[slot] = jnp.broadcast_to(gate, (TOK_TILE, LANES))
            gate_copy(i, slot).start()
            return carry

        lax.fori_loop(0, tok_tiles, gate_tile, 0)
        for i in range(tok_tiles - 2, tok_tiles):
            gate_copy(i, i % 2).wait()

    pl.run_scoped(gate_phase, pltpu.VMEM((2, TOK_TILE, model_dim), jnp.bfloat16), pltpu.VMEM((2, TOK_TILE, LANES), jnp.float32))

    def finish(k, carry):
        for dist in peers:
            out_copy(k, dist).wait_send()
        for dist in peers:
            back_copy(k, dist).wait()
        own_back(k).wait()
        return carry

    lax.fori_loop(0, local_experts, finish, 0)
    for dist in peers:
        ids_copy(dist).wait_send()
        spill_copy(dist).wait_send()
        spill_back(dist).wait()
    own_spill_back().wait()


def split_router(w_router):
    pad = -w_router.shape[1] % LANES
    rest = jnp.pad(w_router, ((0, 0), (0, pad)))
    parts = []
    for _ in range(3):
        piece = lax.reduce_precision(rest, 8, 7)
        parts.append(piece.astype(jnp.bfloat16))
        rest = rest - piece
    return jnp.stack(parts)


def exchange(groups, capacity, cap, spill, tokens, expert_idx, w_router, w_in, w_out):
    local_experts, model_dim, hidden_dim = w_in.shape
    num_experts = groups * local_experts
    tok_count = tokens.shape[0]
    tok_tiles = tok_count // TOK_TILE
    hbm = pl.BlockSpec(memory_space=pl.ANY)
    vmem = pl.BlockSpec(memory_space=pltpu.VMEM)
    per_block = pltpu.SemaphoreType.DMA((groups, local_experts + 1))
    own = pltpu.SemaphoreType.DMA((local_experts + 1,))
    return pl.pallas_call(
        functools.partial(exchange_kernel, groups, num_experts, capacity, cap, spill),
        out_shape=(
            jax.ShapeDtypeStruct((num_experts * cap + groups * spill, model_dim), jnp.bfloat16),
            jax.ShapeDtypeStruct((tok_count, LANES), jnp.float32),
            jax.ShapeDtypeStruct((1,), jnp.int32),
            jax.ShapeDtypeStruct((tok_tiles, 1, TOK_TILE), jnp.int32),
            jax.ShapeDtypeStruct((tok_tiles, 1, TOK_TILE), jnp.int32),
            jax.ShapeDtypeStruct((local_experts, groups * cap, model_dim), jnp.bfloat16),
            jax.ShapeDtypeStruct((groups * spill, model_dim), jnp.bfloat16),
            jax.ShapeDtypeStruct((groups, 8, LANES), jnp.float32),
        ),
        in_specs=[hbm, vmem, vmem, hbm, hbm],
        out_specs=(hbm, hbm, pl.BlockSpec(memory_space=pltpu.SMEM), vmem, vmem, hbm, hbm, hbm),
        scratch_shapes=[
            pltpu.VMEM((local_experts, groups * cap, model_dim), jnp.bfloat16),
            pltpu.VMEM((groups, 8, LANES), jnp.float32),
            pltpu.VMEM((num_experts + groups, LANES), jnp.int32),
            pltpu.VMEM((groups, 8, LANES), jnp.float32),
            pltpu.VMEM((tok_tiles, 1, TOK_TILE), jnp.float32),
            pltpu.SMEM((num_experts + groups, LANES), jnp.int32),
            pltpu.VMEM((groups * spill, model_dim), jnp.bfloat16),
            pltpu.VMEM((groups * spill, model_dim), jnp.bfloat16),
            pltpu.VMEM((groups * spill, LANES), jnp.float32),
            per_block,
            per_block,
            per_block,
            per_block,
            own,
            own,
            pltpu.SemaphoreType.DMA((groups,)),
            pltpu.SemaphoreType.DMA((groups,)),
            pltpu.SemaphoreType.DMA((2, 2)),
            pltpu.SemaphoreType.DMA((tok_tiles,)),
            pltpu.SemaphoreType.DMA((2,)),
            pltpu.SemaphoreType.DMA((2,)),
        ],
        compiler_params=pltpu.CompilerParams(collective_id=0, has_side_effects=True, vmem_limit_bytes=VMEM_LIMIT),
        name="exchange",
    )(tokens, expert_idx.reshape(tok_tiles, 1, TOK_TILE), split_router(w_router), w_in, w_out)


def combine_kernel(in_tile, slot_ref, gate_hbm, src_hbm, y_hbm, src_lin, stage, gates, picked, out_tile, in_sem, gate_sem, out_sem):
    tok_tiles, tile, _ = gates.shape
    model_dim = src_hbm.shape[1]
    pieces = model_dim // LANES
    in_tiles = src_hbm.shape[0] // in_tile
    depth = stage.shape[0]
    out_depth = out_tile.shape[0]

    def load_copy(b):
        slot = lax.rem(b, depth)
        return pltpu.make_async_copy(src_hbm.at[pl.ds(pl.multiple_of(b * in_tile, in_tile), in_tile)], stage.at[slot], in_sem.at[slot])

    def store_copy(i):
        slot = lax.rem(i, out_depth)
        return pltpu.make_async_copy(out_tile.at[slot], y_hbm.at[pl.ds(pl.multiple_of(i * tile, tile), tile)], out_sem.at[slot])

    def start(b, carry):
        load_copy(b).start()
        return carry

    lax.fori_loop(0, min(depth, in_tiles), start, 0)

    def gate_copy(i):
        return pltpu.make_async_copy(gate_hbm.at[pl.ds(pl.multiple_of(i * tile, tile), tile)], gates.at[i], gate_sem.at[i])

    def load(b, carry):
        load_copy(b).wait()
        for j in range(pieces):
            src_lin[pl.ds(b * (in_tile * pieces) + j, in_tile, stride=pieces), :] = stage[lax.rem(b, depth), :, j * LANES:(j + 1) * LANES].astype(jnp.float32)

        @pl.when(b + depth < in_tiles)
        def _():
            load_copy(b + depth).start()

        return carry

    lax.fori_loop(0, in_tiles - depth, load, 0)

    def start_gate(i, carry):
        gate_copy(i).start()
        return carry

    lax.fori_loop(0, tok_tiles, start_gate, 0)
    lax.fori_loop(in_tiles - depth, in_tiles, load, 0)

    def emit(i, carry):
        def pick(q, c):
            for u in range(PICK_UNROLL):
                at = q * PICK_UNROLL + u
                row = slot_ref[i * tile + at]
                picked[pl.ds(at * pieces, pieces), :] = src_lin[pl.ds(row, pieces), :]
            return c

        lax.fori_loop(0, tile // PICK_UNROLL, pick, 0)
        gate_copy(i).wait()

        @pl.when(i >= out_depth)
        def _():
            store_copy(i - out_depth).wait()

        slot = lax.rem(i, out_depth)
        gate = gates[i]
        for j in range(pieces):
            value = picked[pl.ds(j, tile, stride=pieces), :] * gate
            out_tile[slot, :, j * LANES:(j + 1) * LANES] = jnp.where(gate >= 0.0, value, 0.0).astype(jnp.bfloat16)
        store_copy(i).start()
        return carry

    lax.fori_loop(0, tok_tiles, emit, 0)

    def drain(i, carry):
        store_copy(tok_tiles - out_depth + i).wait()
        return carry

    lax.fori_loop(0, out_depth, drain, 0)


def combine(flat_out, slot_index, gate):
    row_count, model_dim = flat_out.shape
    tile = TOK_TILE
    tok_tiles = gate.shape[0] // tile
    pieces = model_dim // LANES
    in_tile = max(n for n in range(16, 513, 16) if row_count % n == 0)
    depth = min(12, row_count // in_tile)
    out_depth = min(6, tok_tiles)
    hbm = pl.BlockSpec(memory_space=pl.ANY)
    return pl.pallas_call(
        functools.partial(combine_kernel, in_tile),
        in_specs=[pl.BlockSpec(memory_space=pltpu.SMEM), hbm, hbm],
        out_specs=hbm,
        scratch_shapes=[
            pltpu.VMEM((row_count * pieces, LANES), jnp.float32),
            pltpu.VMEM((depth, in_tile, model_dim), jnp.bfloat16),
            pltpu.VMEM((tok_tiles, tile, LANES), jnp.float32),
            pltpu.VMEM((tile * pieces, LANES), jnp.float32),
            pltpu.VMEM((out_depth, tile, model_dim), jnp.bfloat16),
            pltpu.SemaphoreType.DMA((depth,)),
            pltpu.SemaphoreType.DMA((tok_tiles,)),
            pltpu.SemaphoreType.DMA((out_depth,)),
        ],
        out_shape=jax.ShapeDtypeStruct((tok_tiles * tile, model_dim), jnp.bfloat16),
        compiler_params=pltpu.CompilerParams(vmem_limit_bytes=VMEM_LIMIT),
        name="combine",
    )(slot_index.reshape(-1), gate, flat_out)


def full_capacity(groups, capacity, tokens, full_slot, gate, w_in, w_out):
    tok_count, model_dim = tokens.shape
    local_experts = w_in.shape[0]
    slots = local_experts * groups * capacity
    slot_index = full_slot.reshape(-1)
    holder = jnp.full((slots + 1,), tok_count, jnp.int32).at[slot_index].set(jnp.arange(tok_count, dtype=jnp.int32))
    buffer = jnp.take(tokens, holder[:-1], axis=0, mode="fill", fill_value=0)
    recv_buf = lax.all_to_all(buffer.reshape(groups, local_experts, capacity, model_dim), "ep", 0, 0, tiled=True)

    def one_expert(operands):
        rows_of, first, second = operands
        hidden_act = jax.nn.relu(jnp.dot(rows_of.reshape(groups * capacity, model_dim), first, preferred_element_type=jnp.float32)).astype(jnp.bfloat16)
        return jnp.dot(hidden_act, second, preferred_element_type=jnp.float32).astype(jnp.bfloat16).reshape(groups, capacity, model_dim)

    expert_rows = lax.map(one_expert, (jnp.swapaxes(recv_buf, 0, 1), w_in, w_out))
    back_buf = lax.all_to_all(jnp.swapaxes(expert_rows, 0, 1), "ep", 0, 0, tiled=True)
    return combine(back_buf.reshape(slots, model_dim), jnp.minimum(full_slot, slots - 1) * (model_dim // LANES), gate)


def solution(mesh):
    groups = mesh.shape["ep"]

    def local_block(tokens, expert_idx, w_router, w_in, w_out):
        tok_count = tokens.shape[0]
        num_experts = w_in.shape[0] * groups
        capacity = (5 * tok_count + 4 * num_experts - 1) // (4 * num_experts)
        main = tok_count // num_experts
        spill = capacity // 2
        back_buf, gate, too_many, slot_index, full_slot, _, _, _ = exchange(groups, capacity, main, spill, tokens, expert_idx, w_router, w_in, w_out)
        return lax.cond(
            too_many[0] > 0,
            lambda: full_capacity(groups, capacity, tokens, full_slot, gate, w_in, w_out),
            lambda: combine(back_buf, slot_index, gate))

    return jax.shard_map(local_block, mesh=mesh, in_specs=(P(("dp", "ep"), None), P(("dp", "ep")), P(None, None), P("ep", None, None), P("ep", None, None)), out_specs=P(("dp", "ep"), None), check_vma=False)
```
